32 devices in a mesh: rep: 1 (over z), head: 4 (over y), seq: 8 (over x, core).
Axes of the slice: x: 4, y: 4, z: 1, core: 2. Of those that a mesh axis runs over, the one named last changes fastest.
The devices are a block of a 4x4x8 slice.
Arguments:
- tokens: bfloat16 [64, 6144], P('rep')
- w_query: bfloat16 [6144, 6144], replicated
- w_key: bfloat16 [6144, 1024], replicated
- w_value: bfloat16 [6144, 1024], replicated
- w_out: bfloat16 [6144, 6144], P(('head', 'seq'))
- k_cache: bfloat16 [64, 2048, 8, 128], P('rep', 'seq', 'head')
- v_cache: bfloat16 [64, 2048, 8, 128], P('rep', 'seq', 'head')
- positions: int32 [64], P('rep')
Outputs:
- output 1: bfloat16 [64, 6144], P('rep')
- output 2: bfloat16 [64, 2048, 8, 128], P('rep', 'seq', 'head')
- output 3: bfloat16 [64, 2048, 8, 128], P('rep', 'seq', 'head')
All inputs are finite; a program needn't handle non-finite values.
Results may differ from the reference program's by a relative error of at most 0.00793011.
Values are sent between devices in bfloat16 or wider.
A program may use at most 768 MiB of HBM per device.

```python
import math
import jax
import jax.numpy as jnp
from jax import lax

BATCH = 64
D_MODEL = 6144
N_HEADS = 48
N_KV = 8
HEAD_DIM = 128
SHARD_LEN = 256
SEQ_LEN = 2048
KEY_SCALE = math.sqrt(math.log(SHARD_LEN / 16))


def setup_inputs(seed: int = 0, part: int = 0) -> dict:
    base_key = jax.random.key(seed)
    part_key = jax.random.fold_in(base_key, part)
    weight_keys = jax.random.split(base_key, 4)
    part_keys = jax.random.split(part_key, 4)
    tokens = jax.random.normal(part_keys[0], (BATCH, D_MODEL), jnp.float32)
    w_query = jax.random.normal(weight_keys[0], (D_MODEL, N_HEADS * HEAD_DIM), jnp.float32) * D_MODEL ** -0.5
    w_key = jax.random.normal(weight_keys[1], (D_MODEL, N_KV * HEAD_DIM), jnp.float32) * (KEY_SCALE * D_MODEL ** -0.5)
    w_value = jax.random.normal(weight_keys[2], (D_MODEL, N_KV * HEAD_DIM), jnp.float32) * D_MODEL ** -0.5
    w_out = jax.random.normal(weight_keys[3], (N_HEADS * HEAD_DIM, D_MODEL), jnp.float32) * (N_HEADS * HEAD_DIM) ** -0.5
    k_cache = jax.random.normal(part_keys[1], (BATCH, SEQ_LEN, N_KV, HEAD_DIM), jnp.float32) * KEY_SCALE
    v_cache = jax.random.normal(part_keys[2], (BATCH, SEQ_LEN, N_KV, HEAD_DIM), jnp.float32)
    positions = jax.random.randint(part_keys[3], (BATCH,), 0, SEQ_LEN, jnp.int32)
    positions = positions.at[0].set(SEQ_LEN - 1)
    return {
        'tokens': tokens.astype(jnp.bfloat16),
        'w_query': w_query.astype(jnp.bfloat16),
        'w_key': w_key.astype(jnp.bfloat16),
        'w_value': w_value.astype(jnp.bfloat16),
        'w_out': w_out.astype(jnp.bfloat16),
        'k_cache': k_cache.astype(jnp.bfloat16),
        'v_cache': v_cache.astype(jnp.bfloat16),
        'positions': positions,
    }


def reference(tokens, w_query, w_key, w_value, w_out, k_cache, v_cache, positions):
    groups = N_HEADS // N_KV
    query = jnp.dot(tokens, w_query, preferred_element_type=jnp.float32).astype(jnp.bfloat16)
    new_key = jnp.dot(tokens, w_key, preferred_element_type=jnp.float32).astype(jnp.bfloat16)
    new_value = jnp.dot(tokens, w_value, preferred_element_type=jnp.float32).astype(jnp.bfloat16)
    query = query.reshape(BATCH, N_KV, groups, HEAD_DIM)
    new_key = new_key.reshape(BATCH, N_KV, HEAD_DIM)
    new_value = new_value.reshape(BATCH, N_KV, HEAD_DIM)
    slot_ids = jnp.arange(SEQ_LEN, dtype=jnp.int32)

    def one_row(row_inputs):
        q_row, key_row, value_row, k_rows, v_rows, pos_row = row_inputs
        is_slot = (slot_ids == pos_row)[:, None, None]
        k_new = jnp.where(is_slot, key_row[None], k_rows)
        v_new = jnp.where(is_slot, value_row[None], v_rows)
        scores = jnp.einsum('kgd,tkd->kgt', q_row.astype(jnp.float32), k_new.astype(jnp.float32)) * HEAD_DIM ** -0.5
        scores = jnp.where(slot_ids <= pos_row, scores, -jnp.inf)
        row_max = jnp.max(scores, axis=-1, keepdims=True)
        weights = jnp.exp(scores - row_max)
        row_sum = jnp.sum(weights, axis=-1, keepdims=True)
        mixed_sum = jnp.einsum('kgt,tkd->kgd', weights.astype(jnp.bfloat16).astype(jnp.float32), v_new.astype(jnp.float32))
        attn_row = (mixed_sum / row_sum).astype(jnp.bfloat16)
        return k_new, v_new, attn_row

    k_out, v_out, attn_rows = lax.map(one_row, (query, new_key, new_value, k_cache, v_cache, positions))
    attn_flat = attn_rows.reshape(BATCH, N_HEADS * HEAD_DIM)
    y_out = jnp.dot(attn_flat, w_out, preferred_element_type=jnp.float32).astype(jnp.bfloat16)
    return y_out, k_out, v_out
```

```python
import functools

import jax
import jax.numpy as jnp
from jax import lax
from jax.experimental import pallas as pl
from jax.experimental.pallas import tpu as pltpu
from jax.sharding import PartitionSpec as P

MESH = pl.DeviceIdType.MESH
BF16 = jnp.bfloat16
F32 = jnp.float32
PAD = 16
NB = 8


def attend(groups, tok, wq, wk, wv, kc, vc, pos, ko, vo, acch, stat,
           wbuf, kb, vb, pj, q2, accs, wsem, ksem, vsem, kosem, vosem):
    head = lax.axis_index('head')
    seq = lax.axis_index('seq')
    batch, rows, dim = kc.shape
    shard = rows // 2
    heads = 2 * groups
    nq = groups
    width = 2 * dim
    steps = batch // NB

    def weight(i):
        if i < nq:
            src = wq.at[:, pl.ds(pl.multiple_of((head * nq + i) * width, width), width)]
        else:
            src = (wk if i == nq else wv).at[:, pl.ds(pl.multiple_of(head * width, width), width)]
        return pltpu.make_async_copy(src, wbuf.at[i], wsem.at[i])

    def block(src, dst, sem, c):
        span = pl.ds(pl.multiple_of(c * NB, NB), NB)
        return pltpu.make_async_copy(src.at[span], dst.at[span], sem.at[c])

    for i in range(nq + 2):
        weight(i).start()
    for c in range(steps):
        block(kc, kb, ksem, c).start()
        block(vc, vb, vsem, c).start()
    q2[...] = jnp.zeros_like(q2)

    def project(i, carry):
        pltpu.make_async_copy(wq.at[:, pl.ds(0, width)], wbuf.at[i], wsem.at[i]).wait()
        out = jnp.dot(tok[...], wbuf[i], preferred_element_type=F32)
        pj[i] = out.astype(BF16).astype(F32)
        return carry

    lax.fori_loop(0, nq + 2, project, 0)
    for h in range(heads):
        q2[pl.ds(h, batch, stride=PAD), :] = pj[h // 2][:, (h % 2) * dim:(h % 2 + 1) * dim]

    row16 = lax.broadcasted_iota(jnp.int32, (16, dim), 0)
    even = (row16 & 1) == 0
    lane = lax.broadcasted_iota(jnp.int32, (PAD, dim), 1)
    col = lax.broadcasted_iota(jnp.int32, (PAD, rows), 1)
    rid = lax.broadcasted_iota(jnp.int32, (PAD, rows), 0)
    slot = col >> 1
    own = jnp.where(rid < groups, 0, jnp.where(rid < heads, 1, 2)) == (col & 1)
    slot = jnp.where(own, slot, jnp.int32(1 << 30))

    def step(c, st):
        def update(buf, which):
            for i in range(NB):
                b = c * NB + i
                t = pos[b] - seq * shard
                inside = (t >= 0) & (t < shard)
                tc = jnp.clip(t, 0, shard - 1)
                start = pl.multiple_of((tc >> 3) * 16, 16)
                hit = ((row16 >> 1) == (tc & 7)) & inside
                new = pj[which, pl.ds(b, 1), :]
                new = jnp.where(even, new[:, :dim], new[:, dim:])
                old = buf[b, pl.ds(start, 16), :].astype(F32)
                buf[b, pl.ds(start, 16), :] = jnp.where(hit, new, old).astype(BF16)

        block(kc, kb, ksem, c).wait()
        update(kb, nq)
        block(kb, ko, kosem, c).start()
        block(vc, vb, vsem, c).wait()
        update(vb, nq + 1)
        block(vb, vo, vosem, c).start()
        for i in range(NB):
            b = c * NB + i
            t = pos[b] - seq * shard
            q = q2[pl.ds(pl.multiple_of(b * PAD, PAD), PAD), :].astype(BF16)
            s = lax.dot_general(q, kb[b], (((1,), (1,)), ((), ())), preferred_element_type=F32)
            s = jnp.where(slot <= t, s * dim ** -0.5, -jnp.inf)
            m = jnp.max(s, axis=-1, keepdims=True)
            w = jnp.exp(s - jnp.where(m == -jnp.inf, 0.0, m))
            l = jnp.sum(w, axis=-1, keepdims=True)
            acc = jnp.dot(w.astype(BF16), vb[b], preferred_element_type=F32)
            accs[pl.ds(pl.multiple_of(b * PAD, PAD), PAD), :] = acc
            st = jnp.where(lane == b, m, jnp.where(lane == b + batch, l, st))
        return st

    stat[...] = lax.fori_loop(0, steps, step, jnp.zeros((PAD, dim), F32))
    for h in range(heads):
        acch[h] = accs[pl.ds(h, batch, stride=PAD), :]
    for c in range(steps):
        block(kb, ko, kosem, c).wait()
        block(vb, vo, vosem, c).wait()


def finish(acch, stat, wo, out, wob, rx, srx, fs, lhs, yp, dx, z, r1, s1, r2, yb,
           osem, ds_s, ds_r, ss_s, ss_r, d_s, d_r, a_s, a_r, b_s, b_r, c_s, c_r, e_s, e_r, f_s, f_r):
    y = lax.axis_index('head')
    s = lax.axis_index('seq')
    ny = lax.axis_size('head')
    ns = lax.axis_size('seq')
    nx = ns // 2
    x = s // 2
    p = lax.rem(s, 2)
    heads, batch, dim = acch.shape
    wrows = wo.shape[0]
    wide = yp.shape[-1]
    half = batch // 2

    def at(yy, xx, pp):
        return {'head': yy, 'seq': xx * 2 + pp}

    partner = at(y, x, 1 - p)

    def on_x(k):
        return at(y, lax.rem(x + k, nx), p)

    def on_y(k):
        return at(lax.rem(y + k, ny), x, p)

    load = pltpu.make_async_copy(wo, wob.at[pl.ds(pl.multiple_of(p * (2 * dim - wrows), 64), wrows), :], osem)
    load.start()
    gap = pl.multiple_of((1 - p) * wrows, 64)
    wob[pl.ds(gap, 2 * dim - wrows), :] = jnp.zeros((2 * dim - wrows, wob.shape[1]), BF16)

    barrier = pltpu.get_barrier_semaphore()
    for k in range(1, ns):
        pl.semaphore_signal(barrier, inc=1, device_id={'head': y, 'seq': lax.rem(s + k, ns)}, device_id_type=MESH)
    for k in range(1, ny):
        pl.semaphore_signal(barrier, inc=1, device_id=on_y(k), device_id_type=MESH)
    pl.semaphore_wait(barrier, ns - 1 + ny - 1)

    def copy(src, dst, send, recv, dev):
        return pltpu.make_async_remote_copy(src_ref=src, dst_ref=dst, send_sem=send, recv_sem=recv,
                                            device_id=dev, device_id_type=MESH)

    def first(dest):
        return (dest // 2) * 3 + lax.rem(dest, 2)

    sends = []
    order = [4, 5, 3, 2, 6, 7, 1]
    for k in order:
        dest = lax.rem(s + k, ns)
        dev = {'head': y, 'seq': dest}
        cp = copy(stat, srx.at[k], ss_s.at[k], ss_r.at[k], dev)
        cp.start()
        sends.append(cp)
        cp = copy(acch.at[pl.ds(first(dest), 2)], rx.at[k], ds_s.at[k], ds_r.at[k], dev)
        cp.start()
        sends.append(cp)
    srx[0] = stat[...]
    fs[...] = jnp.zeros_like(fs)
    for cp in sends:
        cp.wait_recv()

    h0 = first(s)
    tiles = [srx[i, pl.ds(h0, 2), :] for i in range(ns)]
    top = functools.reduce(jnp.maximum, tiles)
    scale = [jnp.exp(t - top) for t in tiles]
    total = functools.reduce(lambda a, b: a + b, [e * pltpu.roll(t, dim // 2, 1) for e, t in zip(scale, tiles)])
    for i in range(ns):
        fs[2 * i:2 * i + 2, :] = scale[i] / total
    ft = jnp.transpose(fs[...])[:batch]
    lane = lax.broadcasted_iota(jnp.int32, (batch, dim), 1)
    for j in range(2):
        acc = ft[:, j:j + 1] * acch[h0 + j]
        for i in range(1, ns):
            acc = acc + ft[:, 2 * i + j:2 * i + j + 1] * rx[i, j]
        keep = (lane >= dim // 2) if j == 0 else (lane < dim // 2)
        keep = keep | (p == j)
        lhs[:, j * dim:(j + 1) * dim] = jnp.where(keep, acc, 0.0).astype(BF16)
    load.wait()

    seq_of = []
    for k in (2, 1, 3, 0):
        seq_of.append((0, k))
        seq_of.append((1, k))

    def block_of(side, k):
        return lax.rem(x + k, nx) if side == 0 else nx + lax.rem(y + k, ny)

    pair = {}
    for side, k in seq_of:
        c = block_of(side, k)
        v = jnp.dot(lhs[...], wob[:, pl.ds(pl.multiple_of(c * wide, wide), wide)], preferred_element_type=F32)
        i = side * 4 + k
        yp[i, 0] = v[:half]
        yp[i, 1] = v[half:]
        cp = copy(yp.at[i, 1 - p], dx.at[i], d_s.at[i], d_r.at[i], partner)
        cp.start()
        pair[side, k] = cp
        sends.append(cp)

    one = {}
    for side, k in seq_of:
        i = side * 4 + k
        pair[side, k].wait_recv()
        z[i] = yp[i, p] + dx[i]
        if k:
            cp = copy(z.at[i], r1.at[i], a_s.at[i], a_r.at[i], on_x(k) if side == 0 else on_y(k))
            cp.start()
            one[side, k] = cp
            sends.append(cp)

    two = {}
    for side in range(2):
        base = side * 4
        for k in range(1, 4):
            one[side, k].wait_recv()
        v = z[base] + r1[base + 1] + r1[base + 2] + r1[base + 3]
        for r in range(4):
            s1[side, r] = v[8 * r:8 * r + 8]
        for k in range(1, 4):
            dest = lax.rem(y + k, ny) if side == 0 else lax.rem(x + k, nx)
            cp = copy(s1.at[side, dest], r2.at[base + k], b_s.at[base + k], b_r.at[base + k],
                      on_y(k) if side == 0 else on_x(k))
            cp.start()
            two[side, k] = cp
            sends.append(cp)

    three = {}
    for side in range(2):
        base = side * 4
        mine = y if side == 0 else x
        c = block_of(side, 0)
        for k in range(1, 4):
            two[side, k].wait_recv()
        v = s1[side, mine] + r2[base + 1] + r2[base + 2] + r2[base + 3]
        row = 4 * p + mine
        yb[c, row] = v.astype(BF16)
        for k in range(1, 4):
            cp = copy(yb.at[c, row], yb.at[c, row], c_s.at[base + k], c_r.at[base + k],
                      on_y(k) if side == 0 else on_x(k))
            cp.start()
            three[side, k] = cp
            sends.append(cp)

    def mirror(side, k):
        c = block_of(side, k)
        part = yb.at[c, pl.ds(4 * p, 4)]
        i = side * 4 + k
        cp = copy(part, part, f_s.at[i], f_r.at[i], partner)
        cp.start()
        sends.append(cp)
        return cp

    four = {}
    last = []
    for side in range(2):
        base = side * 4
        c = block_of(side, 0)
        for k in range(1, 4):
            three[side, k].wait_recv()
        part = yb.at[c, pl.ds(4 * p, 4)]
        for k in range(1, 4):
            cp = copy(part, part, e_s.at[base + k], e_r.at[base + k], on_x(k) if side == 0 else on_y(k))
            cp.start()
            four[side, k] = cp
            sends.append(cp)
        last.append(mirror(side, 0))
    for k in (1, 3, 2):
        for side in range(2):
            four[side, k].wait_recv()
            last.append(mirror(side, 4 - k))
    for cp in last:
        cp.wait_recv()
    for c in range(2 * nx):
        out[:, :, c * wide:(c + 1) * wide] = yb[c]
    for cp in sends:
        cp.wait_send()


def solution(mesh):
    cache_spec = P('rep', 'seq', 'head', None)

    def local_step(tokens, w_query, w_key, w_value, w_out, k_cache, v_cache, positions):
        batch, shard, kv, dim = k_cache.shape
        model = tokens.shape[1]
        groups = w_query.shape[1] // w_key.shape[1]
        heads = kv * groups
        rows = shard * kv
        flat = (batch, rows, dim)
        anyspec = pl.BlockSpec(memory_space=pl.ANY)
        vspec = pl.BlockSpec(memory_space=pltpu.VMEM)
        steps = batch // NB
        dma = pltpu.SemaphoreType.DMA
        k_new, v_new, acc, stat = pl.pallas_call(
            functools.partial(attend, groups),
            out_shape=(jax.ShapeDtypeStruct(flat, BF16), jax.ShapeDtypeStruct(flat, BF16),
                       jax.ShapeDtypeStruct((heads, batch, dim), F32), jax.ShapeDtypeStruct((PAD, dim), F32)),
            in_specs=[vspec, anyspec, anyspec, anyspec, anyspec, anyspec, pl.BlockSpec(memory_space=pltpu.SMEM)],
            out_specs=(anyspec, anyspec, vspec, vspec),
            scratch_shapes=[
                pltpu.VMEM((groups + 2, model, kv * dim), BF16),
                pltpu.VMEM(flat, BF16),
                pltpu.VMEM(flat, BF16),
                pltpu.VMEM((groups + 2, batch, kv * dim), F32),
                pltpu.VMEM((batch * PAD, dim), F32),
                pltpu.VMEM((batch * PAD, dim), F32),
                dma((groups + 2,)), dma((steps,)), dma((steps,)), dma((steps,)), dma((steps,)),
            ],
            compiler_params=pltpu.CompilerParams(vmem_limit_bytes=56 << 20),
            name='attend',
        )(tokens, w_query, w_key, w_value, k_cache.reshape(flat), v_cache.reshape(flat), positions)

        wide = model // 8
        half = batch // 2
        ns = lax.axis_size('seq')
        y = pl.pallas_call(
            finish,
            out_shape=jax.ShapeDtypeStruct((8, 8, model), BF16),
            in_specs=[vspec, vspec, anyspec],
            out_specs=vspec,
            scratch_shapes=[
                pltpu.VMEM((2 * dim, model), BF16),
                pltpu.VMEM((ns, 2, batch, dim), F32),
                pltpu.VMEM((ns, PAD, dim), F32),
                pltpu.VMEM((dim, dim), F32),
                pltpu.VMEM((batch, 2 * dim), BF16),
                pltpu.VMEM((8, 2, half, wide), F32),
                pltpu.VMEM((8, half, wide), F32),
                pltpu.VMEM((8, half, wide), F32),
                pltpu.VMEM((8, half, wide), F32),
                pltpu.VMEM((2, 4, 8, wide), F32),
                pltpu.VMEM((8, 8, wide), F32),
                pltpu.VMEM((8, 8, 8, wide), BF16),
                dma,
            ] + [dma((8,))] * 16,
            compiler_params=pltpu.CompilerParams(collective_id=0, has_side_effects=True, vmem_limit_bytes=32 << 20),
            name='finish',
        )(acc, stat, w_out)
        return y.reshape(batch, model), k_new.reshape(k_cache.shape), v_new.reshape(v_cache.shape)

    return jax.shard_map(
        local_step,
        mesh=mesh,
        in_specs=(P('rep', None), P(), P(), P(), P(('head', 'seq'), None), cache_spec, cache_spec, P('rep')),
        out_specs=(P('rep', None), cache_spec, cache_spec),
        check_vma=False,
    )
```

```python
import functools

import jax
import jax.numpy as jnp
from jax import lax
from jax.experimental import pallas as pl
from jax.experimental.pallas import tpu as pltpu
from jax.sharding import PartitionSpec as P

MESH = pl.DeviceIdType.MESH
BF16 = jnp.bfloat16
F32 = jnp.float32
PAD = 16
NB = 16


def project(groups, tokens, wq, wk, wv, kc, vc, pj, kb, vb, tok, wbuf, tsem, wsem, ssem, rsem, ksem, vsem):
    head = lax.axis_index('head')
    s = lax.axis_index('seq')
    p = lax.rem(s, 2)
    width = pj.shape[-1]
    per = wbuf.shape[0]
    partner = {'head': head, 'seq': s + 1 - 2 * p}

    def load(i, src, block):
        return pltpu.make_async_copy(src.at[:, pl.ds(pl.multiple_of(block * width, width), width)], wbuf.at[i], wsem.at[i])

    first = pltpu.make_async_copy(tokens, tok, tsem)
    first.start()
    for i in range(per):
        @pl.when(p == 0)
        def _():
            load(i, wq, head * groups + i).start()

        @pl.when(p == 1)
        def _():
            if per + i < groups:
                load(i, wq, head * groups + per + i).start()
            else:
                load(i, wk if per + i == groups else wv, head).start()

    caches = [pltpu.make_async_copy(kc, kb, ksem), pltpu.make_async_copy(vc, vb, vsem)]
    for cp in caches:
        cp.start()
    barrier = pltpu.get_barrier_semaphore()
    pl.semaphore_signal(barrier, inc=1, device_id=partner, device_id_type=MESH)
    pl.semaphore_wait(barrier, 1)
    sends = []
    first.wait()
    for i in range(per):
        load(i, wq, 0).wait()
        slot = p * per + i
        pj[slot] = jnp.dot(tok[...], wbuf[i], preferred_element_type=F32).astype(BF16)
        cp = pltpu.make_async_remote_copy(src_ref=pj.at[slot], dst_ref=pj.at[slot], send_sem=ssem.at[i],
                                          recv_sem=rsem.at[i], device_id=partner, device_id_type=MESH)
        cp.start()
        sends.append(cp)
    for cp in sends:
        cp.wait_recv()
    for cp in sends:
        cp.wait_send()
    for cp in caches:
        cp.wait()


def attend(groups, pj, kin, vin, pos, ko, vo, kb, vb, acch, stat, q2, nkv, accs, osem):
    seq = lax.axis_index('seq')
    batch, rows, dim = kb.shape
    shard = rows // 2
    heads = 2 * groups
    steps = batch // NB
    q2[...] = jnp.zeros_like(q2)
    for h in range(heads):
        q2[pl.ds(h, batch, stride=PAD), :] = pj[h // 2][:, (h % 2) * dim:(h % 2 + 1) * dim].astype(F32)
    nkv[0] = pj[groups].astype(F32)
    nkv[1] = pj[groups + 1].astype(F32)

    row16 = lax.broadcasted_iota(jnp.int32, (16, dim), 0)
    even = (row16 & 1) == 0
    lanes = NB * PAD
    lane = lax.broadcasted_iota(jnp.int32, (8, lanes), 1)
    sub = lax.broadcasted_iota(jnp.int32, (8, lanes), 0)
    hl = lane & (PAD - 1)
    match = jnp.where(hl < groups, 0, jnp.where(hl < heads, 1, 2)) == (sub & 1)
    tile = lax.broadcasted_iota(jnp.int32, (rows // 8, 8, lanes), 0) * 4

    def out(j, c):
        span = pl.ds(pl.multiple_of(c * NB, NB), NB)
        src, dst = ((kb, ko), (vb, vo))[j]
        return pltpu.make_async_copy(src.at[span], dst.at[span], osem.at[j, c])

    def step(c, carry):
        limit = jnp.zeros((8, lanes), jnp.int32)
        for i in range(NB):
            b = c * NB + i
            t = pos[b] - seq * shard
            limit = jnp.where(lane // PAD == i, t, limit)
            inside = (t >= 0) & (t < shard)
            tc = jnp.clip(t, 0, shard - 1)
            start = pl.multiple_of((tc >> 3) * 16, 16)
            hit = ((row16 >> 1) == (tc & 7)) & inside
            for j, buf in enumerate((kb, vb)):
                new = nkv[j, pl.ds(b, 1), :]
                new = jnp.where(even, new[:, :dim], new[:, dim:])
                old = buf[b, pl.ds(start, 16), :].astype(F32)
                buf[b, pl.ds(start, 16), :] = jnp.where(hit, new, old).astype(BF16)
        out(0, c).start()
        out(1, c).start()
        edge = jnp.where(match, limit, -1) - (sub >> 1)
        qt = jnp.transpose(q2[pl.ds(pl.multiple_of(c * lanes, lanes), lanes), :]).astype(BF16)
        ql = lax.broadcasted_iota(jnp.int32, (dim, lanes), 1) // PAD
        s = jnp.zeros((rows, lanes), F32)
        for j in range(NB // 2):
            b = c * NB + 2 * j
            lhs = jnp.concatenate([kb[b], kb[b + 1]], axis=1)
            zero = jnp.zeros_like(qt)
            rhs = jnp.concatenate([jnp.where(ql == 2 * j, qt, zero), jnp.where(ql == 2 * j + 1, qt, zero)], axis=0)
            s = s + jnp.dot(lhs, rhs, preferred_element_type=F32)
        s = s.reshape(rows // 8, 8, lanes) * dim ** -0.5
        s = jnp.where(tile <= edge[None], s, -jnp.inf)
        m = jnp.max(jnp.max(s, axis=0), axis=0, keepdims=True)
        w = jnp.exp(s - jnp.where(m == -jnp.inf, 0.0, m)[None])
        l = jnp.sum(jnp.sum(w, axis=0), axis=0, keepdims=True)
        for r in range(lanes // dim):
            stat[pl.ds(c * (lanes // dim) + r, 1), :] = m[:, r * dim:(r + 1) * dim]
            stat[pl.ds(8 + c * (lanes // dim) + r, 1), :] = l[:, r * dim:(r + 1) * dim]
        wt = jnp.transpose(w.reshape(rows, lanes)).astype(BF16)
        for j in range(NB // 2):
            b = c * NB + 2 * j
            rhs = jnp.concatenate([vb[b], vb[b + 1]], axis=1)
            a = jnp.dot(wt[2 * PAD * j:2 * PAD * (j + 1)], rhs, preferred_element_type=F32)
            accs[pl.ds(pl.multiple_of(b * PAD, PAD), PAD), :] = a[:PAD, :dim]
            accs[pl.ds(pl.multiple_of(b * PAD + PAD, PAD), PAD), :] = a[PAD:, dim:]
        return carry

    lax.fori_loop(0, steps, step, 0)
    for h in range(heads):
        acch[h] = accs[pl.ds(h, batch, stride=PAD), :]
    for c in range(steps):
        out(0, c).wait()
        out(1, c).wait()


def finish(acch, stat, wo, out, wob, rx, srx, fs, lhs, yp, dx, z, r1, s1, r2, yb,
           osem, ds_s, ds_r, ss_s, ss_r, d_s, d_r, a_s, a_r, b_s, b_r, c_s, c_r, e_s, e_r, f_s, f_r):
    y = lax.axis_index('head')
    s = lax.axis_index('seq')
    ny = lax.axis_size('head')
    ns = lax.axis_size('seq')
    nx = ns // 2
    x = s // 2
    p = lax.rem(s, 2)
    heads, batch, dim = acch.shape
    wrows = wo.shape[0]
    wide = yp.shape[-1]
    half = batch // 2

    def at(yy, xx, pp):
        return {'head': yy, 'seq': xx * 2 + pp}

    partner = at(y, x, 1 - p)

    def on_x(k):
        return at(y, lax.rem(x + k, nx), p)

    def on_y(k):
        return at(lax.rem(y + k, ny), x, p)

    load = pltpu.make_async_copy(wo, wob.at[pl.ds(pl.multiple_of(p * (2 * dim - wrows), 64), wrows), :], osem)
    load.start()
    gap = pl.multiple_of((1 - p) * wrows, 64)
    wob[pl.ds(gap, 2 * dim - wrows), :] = jnp.zeros((2 * dim - wrows, wob.shape[1]), BF16)

    barrier = pltpu.get_barrier_semaphore()
    for k in range(1, ns):
        pl.semaphore_signal(barrier, inc=1, device_id={'head': y, 'seq': lax.rem(s + k, ns)}, device_id_type=MESH)
    for k in range(1, ny):
        pl.semaphore_signal(barrier, inc=1, device_id=on_y(k), device_id_type=MESH)
    pl.semaphore_wait(barrier, ns - 1 + ny - 1)

    def copy(src, dst, send, recv, dev):
        return pltpu.make_async_remote_copy(src_ref=src, dst_ref=dst, send_sem=send, recv_sem=recv,
                                            device_id=dev, device_id_type=MESH)

    def first(dest):
        return (dest // 2) * 3 + lax.rem(dest, 2)

    sends = []
    order = [4, 5, 3, 2, 6, 7, 1]
    for k in order:
        dest = lax.rem(s + k, ns)
        dev = {'head': y, 'seq': dest}
        cp = copy(stat, srx.at[k], ss_s.at[k], ss_r.at[k], dev)
        cp.start()
        sends.append(cp)
        cp = copy(acch.at[pl.ds(first(dest), 2)], rx.at[k], ds_s.at[k], ds_r.at[k], dev)
        cp.start()
        sends.append(cp)
    srx[0] = stat[...]
    fs[...] = jnp.zeros_like(fs)
    for cp in sends:
        cp.wait_recv()

    h0 = first(s)
    rows = batch // 8
    peaks = [srx[i, :rows] for i in range(ns)]
    top = functools.reduce(jnp.maximum, peaks)
    scale = [jnp.exp(m - top) for m in peaks]
    total = functools.reduce(lambda a, b: a + b, [e * srx[i, rows:] for i, e in enumerate(scale)])
    for i in range(ns):
        fs[i * rows:(i + 1) * rows, :] = scale[i] / total
    fs[...] = jnp.transpose(fs[...])
    lane = lax.broadcasted_iota(jnp.int32, (batch, dim), 1)
    for j in range(2):
        col = fs[pl.ds(h0 + j, 8, stride=PAD), :]
        parts = []
        for c in range(rows):
            acc = col[:, c:c + 1] * acch[h0 + j, 8 * c:8 * c + 8]
            for i in range(1, ns):
                acc = acc + col[:, i * rows + c:i * rows + c + 1] * rx[i, j, 8 * c:8 * c + 8]
            parts.append(acc)
        acc = jnp.concatenate(parts, axis=0)
        keep = (lane >= dim // 2) if j == 0 else (lane < dim // 2)
        keep = keep | (p == j)
        lhs[:, j * dim:(j + 1) * dim] = jnp.where(keep, acc, 0.0).astype(BF16)
    load.wait()

    seq_of = []
    for k in (2, 1, 3, 0):
        seq_of.append((0, k))
        seq_of.append((1, k))

    def block_of(side, k):
        return lax.rem(x + k, nx) if side == 0 else nx + lax.rem(y + k, ny)

    pair = {}
    for side, k in seq_of:
        c = block_of(side, k)
        v = jnp.dot(lhs[...], wob[:, pl.ds(pl.multiple_of(c * wide, wide), wide)], preferred_element_type=F32)
        i = side * 4 + k
        yp[i, 0] = v[:half]
        yp[i, 1] = v[half:]
        cp = copy(yp.at[i, 1 - p], dx.at[i], d_s.at[i], d_r.at[i], partner)
        cp.start()
        pair[side, k] = cp
        sends.append(cp)

    one = {}
    for side, k in seq_of:
        i = side * 4 + k
        pair[side, k].wait_recv()
        z[i] = yp[i, p] + dx[i]
        if k:
            cp = copy(z.at[i], r1.at[i], a_s.at[i], a_r.at[i], on_x(k) if side == 0 else on_y(k))
            cp.start()
            one[side, k] = cp
            sends.append(cp)

    two = {}
    for side in range(2):
        base = side * 4
        for k in range(1, 4):
            one[side, k].wait_recv()
        v = z[base] + r1[base + 1] + r1[base + 2] + r1[base + 3]
        for r in range(4):
            s1[side, r] = v[8 * r:8 * r + 8]
        for k in range(1, 4):
            dest = lax.rem(y + k, ny) if side == 0 else lax.rem(x + k, nx)
            cp = copy(s1.at[side, dest], r2.at[base + k], b_s.at[base + k], b_r.at[base + k],
                      on_y(k) if side == 0 else on_x(k))
            cp.start()
            two[side, k] = cp
            sends.append(cp)

    three = {}
    for side in range(2):
        base = side * 4
        mine = y if side == 0 else x
        c = block_of(side, 0)
        for k in range(1, 4):
            two[side, k].wait_recv()
        v = s1[side, mine] + r2[base + 1] + r2[base + 2] + r2[base + 3]
        row = 4 * p + mine
        yb[c, row] = v.astype(BF16)
        for k in range(1, 4):
            cp = copy(yb.at[c, row], yb.at[c, row], c_s.at[base + k], c_r.at[base + k],
                      on_y(k) if side == 0 else on_x(k))
            cp.start()
            three[side, k] = cp
            sends.append(cp)

    def mirror(side, k):
        c = block_of(side, k)
        part = yb.at[c, pl.ds(4 * p, 4)]
        i = side * 4 + k
        cp = copy(part, part, f_s.at[i], f_r.at[i], partner)
        cp.start()
        sends.append(cp)
        return cp

    four = {}
    last = []
    for side in range(2):
        base = side * 4
        c = block_of(side, 0)
        for k in range(1, 4):
            three[side, k].wait_recv()
        part = yb.at[c, pl.ds(4 * p, 4)]
        for k in range(1, 4):
            cp = copy(part, part, e_s.at[base + k], e_r.at[base + k], on_x(k) if side == 0 else on_y(k))
            cp.start()
            four[side, k] = cp
            sends.append(cp)
        last.append(mirror(side, 0))
    for k in (1, 3, 2):
        for side in range(2):
            four[side, k].wait_recv()
            last.append(mirror(side, 4 - k))
    for cp in last:
        cp.wait_recv()
    for c in range(2 * nx):
        out[:, :, c * wide:(c + 1) * wide] = yb[c]
    for cp in sends:
        cp.wait_send()


def solution(mesh):
    cache_spec = P('rep', 'seq', 'head', None)

    def local_step(tokens, w_query, w_key, w_value, w_out, k_cache, v_cache, positions):
        batch, shard, kv, dim = k_cache.shape
        model = tokens.shape[1]
        groups = w_query.shape[1] // w_key.shape[1]
        heads = kv * groups
        rows = shard * kv
        flat = (batch, rows, dim)
        hspec = pl.BlockSpec(memory_space=pltpu.HBM)
        anyspec = pl.BlockSpec(memory_space=pl.ANY)
        vspec = pl.BlockSpec(memory_space=pltpu.VMEM)
        dma = pltpu.SemaphoreType.DMA
        cache = jax.ShapeDtypeStruct(flat, BF16)
        blocks = groups + 2
        per = blocks // 2
        proj, kb, vb = pl.pallas_call(
            functools.partial(project, groups),
            out_shape=(jax.ShapeDtypeStruct((blocks, batch, kv * dim), BF16), cache, cache),
            in_specs=[hspec] * 6,
            out_specs=(vspec,) * 3,
            scratch_shapes=[pltpu.VMEM(tokens.shape, BF16), pltpu.VMEM((per, model, kv * dim), BF16), dma,
                            dma((per,)), dma((per,)), dma((per,)), dma, dma],
            compiler_params=pltpu.CompilerParams(collective_id=1, has_side_effects=True, vmem_limit_bytes=34 << 20),
            cost_estimate=pl.CostEstimate(flops=10**10, bytes_accessed=30 * 10**6, transcendentals=0),
            name='project',
        )(tokens, w_query, w_key, w_value, k_cache.reshape(flat), v_cache.reshape(flat))
        k_new, v_new, _, _, acc, stat = pl.pallas_call(
            functools.partial(attend, groups),
            out_shape=(cache, cache, cache, cache, jax.ShapeDtypeStruct((heads, batch, dim), F32),
                       jax.ShapeDtypeStruct((PAD, dim), F32)),
            in_specs=[vspec, vspec, vspec, pl.BlockSpec(memory_space=pltpu.SMEM)],
            out_specs=(hspec, hspec, vspec, vspec, vspec, vspec),
            input_output_aliases={1: 2, 2: 3},
            scratch_shapes=[pltpu.VMEM((batch * PAD, dim), F32), pltpu.VMEM((2, batch, kv * dim), F32),
                            pltpu.VMEM((batch * PAD, dim), F32), dma((2, batch // NB))],
            compiler_params=pltpu.CompilerParams(vmem_limit_bytes=24 << 20),
            cost_estimate=pl.CostEstimate(flops=10**10, bytes_accessed=17 * 10**6, transcendentals=0),
            name='attend',
        )(proj, kb, vb, positions)

        wide = model // 8
        half = batch // 2
        ns = lax.axis_size('seq')
        y = pl.pallas_call(
            finish,
            out_shape=jax.ShapeDtypeStruct((8, 8, model), BF16),
            in_specs=[vspec, vspec, anyspec],
            out_specs=vspec,
            scratch_shapes=[
                pltpu.VMEM((2 * dim, model), BF16),
                pltpu.VMEM((ns, 2, batch, dim), F32),
                pltpu.VMEM((ns, PAD, dim), F32),
                pltpu.VMEM((dim, dim), F32),
                pltpu.VMEM((batch, 2 * dim), BF16),
                pltpu.VMEM((8, 2, half, wide), F32),
                pltpu.VMEM((8, half, wide), F32),
                pltpu.VMEM((8, half, wide), F32),
                pltpu.VMEM((8, half, wide), F32),
                pltpu.VMEM((2, 4, 8, wide), F32),
                pltpu.VMEM((8, 8, wide), F32),
                pltpu.VMEM((8, 8, 8, wide), BF16),
                dma,
            ] + [dma((8,))] * 16,
            compiler_params=pltpu.CompilerParams(collective_id=0, has_side_effects=True, vmem_limit_bytes=32 << 20),
            name='finish',
        )(acc, stat, w_out)
        return y.reshape(batch, model), k_new.reshape(k_cache.shape), v_new.reshape(v_cache.shape)

    return jax.shard_map(
        local_step,
        mesh=mesh,
        in_specs=(P('rep', None), P(), P(), P(), P(('head', 'seq'), None), cache_spec, cache_spec, P('rep')),
        out_specs=(P('rep', None), cache_spec, cache_spec),
        check_vma=False,
    )
```

```python
import functools

import jax
import jax.numpy as jnp
from jax import lax
from jax.experimental import pallas as pl
from jax.experimental.pallas import tpu as pltpu
from jax.sharding import PartitionSpec as P

MESH = pl.DeviceIdType.MESH
BF16 = jnp.bfloat16
F32 = jnp.float32
PAD = 16
NB = 16
NC = 2


def project(groups, tokens, wq, wk, wv, kc, vc, pj, kb, vb, tok, wbuf, tsem, wsem, ssem, rsem, ksem, vsem):
    head = lax.axis_index('head')
    s = lax.axis_index('seq')
    ns = lax.axis_size('seq')
    parts, depth, width = wbuf.shape

    def load(i, src, block):
        rows = pl.ds(i * depth, depth)
        return pltpu.make_async_copy(src.at[rows, pl.ds(pl.multiple_of(block * width, width), width)], wbuf.at[i], wsem.at[i])

    first = pltpu.make_async_copy(tokens, tok, tsem)
    first.start()
    for i in range(parts):
        @pl.when(s < groups)
        def _():
            load(i, wq, head * groups + s).start()

        @pl.when(s == groups)
        def _():
            load(i, wk, head).start()

        @pl.when(s == groups + 1)
        def _():
            load(i, wv, head).start()

    caches = [pltpu.make_async_copy(kc, kb, ksem), pltpu.make_async_copy(vc, vb, vsem)]
    for cp in caches:
        cp.start()
    barrier = pltpu.get_barrier_semaphore()
    for k in range(1, ns):
        pl.semaphore_signal(barrier, inc=1, device_id={'head': head, 'seq': lax.rem(s + k, ns)}, device_id_type=MESH)
    first.wait()
    acc = jnp.zeros((tok.shape[0], width), F32)
    for i in range(parts):
        load(i, wq, 0).wait()
        acc = acc + jnp.dot(tok[:, i * depth:(i + 1) * depth], wbuf[i], preferred_element_type=F32)
    pj[s] = acc.astype(BF16)
    pl.semaphore_wait(barrier, ns - 1)
    sends = []
    for k in (4, 5, 3, 2, 6, 7, 1):
        cp = pltpu.make_async_remote_copy(src_ref=pj.at[s], dst_ref=pj.at[s], send_sem=ssem.at[k], recv_sem=rsem.at[k],
                                          device_id={'head': head, 'seq': lax.rem(s + k, ns)}, device_id_type=MESH)
        cp.start()
        sends.append(cp)
    for cp in sends:
        cp.wait_recv()
    for cp in sends:
        cp.wait_send()
    for cp in caches:
        cp.wait()


def attend(groups, pj, kin, vin, pos, ko, vo, kb, vb, acch, stat, q2, nkv, accs, sb, osem):
    seq = lax.axis_index('seq')
    batch, rows, dim = kb.shape
    shard = rows // 2
    heads = 2 * groups
    steps = batch // NB
    q2[...] = jnp.zeros_like(q2)
    for h in range(heads):
        q2[pl.ds(h, batch, stride=PAD), :] = pj[h // 2][:, (h % 2) * dim:(h % 2 + 1) * dim].astype(F32)
    nkv[0] = pj[groups].astype(F32)
    nkv[1] = pj[groups + 1].astype(F32)

    row16 = lax.broadcasted_iota(jnp.int32, (16, dim), 0)
    even = (row16 & 1) == 0
    lanes = NB * PAD
    lane = lax.broadcasted_iota(jnp.int32, (8, lanes), 1)
    sub = lax.broadcasted_iota(jnp.int32, (8, lanes), 0)
    hl = lane & (PAD - 1)
    match = jnp.where(hl < groups, 0, jnp.where(hl < heads, 1, 2)) == (sub & 1)
    tile = lax.broadcasted_iota(jnp.int32, (rows // 8, 8, lanes), 0) * 4

    def out(j, c):
        span = pl.ds(pl.multiple_of(c * NB, NB), NB)
        src, dst = ((kb, ko), (vb, vo))[j]
        return pltpu.make_async_copy(src.at[span], dst.at[span], osem.at[j, c])

    def refresh(c, carry):
        fresh = []
        for i in range(NB):
            b = c * NB + i
            t = pos[b] - seq * shard
            inside = (t >= 0) & (t < shard)
            tc = jnp.clip(t, 0, shard - 1)
            start = pl.multiple_of((tc >> 3) * 16, 16)
            hit = ((row16 >> 1) == (tc & 7)) & inside
            for j, buf in enumerate((kb, vb)):
                new = nkv[j, pl.ds(b, 1), :]
                new = jnp.where(even, new[:, :dim], new[:, dim:])
                old = buf[b, pl.ds(start, 16), :].astype(F32)
                fresh.append((buf, b, start, jnp.where(hit, new, old).astype(BF16)))
        for buf, b, start, value in fresh:
            buf[b, pl.ds(start, 16), :] = value
        out(0, c).start()
        out(1, c).start()
        return carry

    lax.fori_loop(0, steps, refresh, 0)
    ql = lax.broadcasted_iota(jnp.int32, (dim, lanes), 1) // PAD

    def scores(c):
        qt = jnp.transpose(q2[c * lanes:(c + 1) * lanes, :]).astype(BF16)
        zero = jnp.zeros_like(qt)
        s = jnp.zeros((rows, lanes), F32)
        for j in range(NB // 2):
            b = c * NB + 2 * j
            lhs = jnp.concatenate([kb[b], kb[b + 1]], axis=1)
            rhs = jnp.concatenate([jnp.where(ql == 2 * j, qt, zero), jnp.where(ql == 2 * j + 1, qt, zero)], axis=0)
            s = s + jnp.dot(lhs, rhs, preferred_element_type=F32)
        sb[c % 2] = s

    def mix(c):
        limit = jnp.zeros((8, lanes), jnp.int32)
        for i in range(NB):
            limit = jnp.where(lane // PAD == i, pos[c * NB + i] - seq * shard, limit)
        edge = jnp.where(match, limit, -1) - (sub >> 1)
        s = sb[c % 2].reshape(rows // 8, 8, lanes) * dim ** -0.5
        s = jnp.where(tile <= edge[None], s, -jnp.inf)
        m = jnp.max(jnp.max(s, axis=0), axis=0, keepdims=True)
        w = jnp.exp(s - jnp.where(m == -jnp.inf, 0.0, m)[None])
        l = jnp.sum(jnp.sum(w, axis=0), axis=0, keepdims=True)
        for r in range(lanes // dim):
            g = c * (lanes // dim) + r
            g = g // 4 * 8 + g % 4
            stat[g:g + 1, :] = m[:, r * dim:(r + 1) * dim]
            stat[g + 4:g + 5, :] = l[:, r * dim:(r + 1) * dim]
        wt = jnp.transpose(w.reshape(rows, lanes).astype(BF16))
        for j in range(NB // 2):
            b = c * NB + 2 * j
            rhs = jnp.concatenate([vb[b], vb[b + 1]], axis=1)
            a = jnp.dot(wt[2 * PAD * j:2 * PAD * (j + 1)], rhs, preferred_element_type=F32)
            accs[b * PAD:(b + 1) * PAD, :] = a[:PAD, :dim]
            accs[(b + 1) * PAD:(b + 2) * PAD, :] = a[PAD:, dim:]

    scores(0)
    for c in range(steps):
        if c + 1 < steps:
            scores(c + 1)
        mix(c)
    for h in range(heads):
        acch[h] = accs[pl.ds(h, batch, stride=PAD), :]
    for c in range(steps):
        out(0, c).wait()
        out(1, c).wait()


def finish(acch, stat, wo, out, wob, rx, srx, fs, lhs, z, r1, s1, r2, yb,
           osem, w_s, w_r, d_s, d_r, t_s, t_r, a_s, a_r, b_s, b_r, c_s, c_r, e_s, e_r, f_s, f_r):
    y = lax.axis_index('head')
    s = lax.axis_index('seq')
    ny = lax.axis_size('head')
    ns = lax.axis_size('seq')
    nx = ns // 2
    x = s // 2
    p = lax.rem(s, 2)
    heads, batch, dim = acch.shape
    wrows = wo.shape[0]
    nc, per, step = rx.shape[1:4]
    half = nc * step
    wide = z.shape[-1]
    short = wide // 2

    def on_x(k):
        return {'head': y, 'seq': lax.rem(x + k, nx) * 2 + p}

    def on_y(k):
        return {'head': lax.rem(y + k, ny), 'seq': s}

    def copy(src, dst, send, recv, dev):
        return pltpu.make_async_remote_copy(src_ref=src, dst_ref=dst, send_sem=send, recv_sem=recv,
                                            device_id=dev, device_id_type=MESH)

    partner = {'head': y, 'seq': x * 2 + 1 - p}
    mine = wob.at[pl.ds(pl.multiple_of(p * wrows, wrows), wrows), :]
    load = pltpu.make_async_copy(wo, mine, osem)
    load.start()

    barrier = pltpu.get_barrier_semaphore()
    for k in range(1, ns):
        pl.semaphore_signal(barrier, inc=1, device_id={'head': y, 'seq': lax.rem(s + k, ns)}, device_id_type=MESH)
    for k in range(1, ny):
        pl.semaphore_signal(barrier, inc=1, device_id=on_y(k), device_id_type=MESH)
    pl.semaphore_wait(barrier, ns - 1 + ny - 1)

    sends = []

    def go(*a):
        cp = copy(*a)
        cp.start()
        sends.append(cp)
        return cp

    stats, parts = [], {c: [] for c in range(nc)}
    for c in range(nc):
        for k in (4, 5, 3, 2, 6, 7, 1):
            dest = lax.rem(s + k, ns)
            dev = {'head': y, 'seq': dest}
            side = lax.rem(dest, 2)
            if c == 0:
                rows = pl.ds(pl.multiple_of(side * 8, 8), 8)
                stats.append(go(stat.at[rows], srx.at[k], t_s.at[k], t_r.at[k], dev))
            rows = pl.ds(pl.multiple_of(side * half + c * step, step), step)
            parts[c].append(go(acch.at[pl.ds((dest // 2) * per, per), rows], rx.at[k, c], d_s.at[c, k], d_r.at[c, k], dev))
    wcopy = go(wo, mine, w_s, w_r, partner)
    srx[0] = stat[pl.ds(pl.multiple_of(p * 8, 8), 8)]
    fs[...] = jnp.zeros_like(fs)
    for cp in stats:
        cp.wait_recv()
    n8 = half // 8
    top = functools.reduce(jnp.maximum, [srx[i, :n8] for i in range(ns)])
    scale = [jnp.exp(srx[i, :n8] - top) for i in range(ns)]
    total = functools.reduce(lambda a, b: a + b, [e * srx[i, n8:] for i, e in enumerate(scale)])
    for i in range(ns):
        fs[i * n8:(i + 1) * n8, :] = scale[i] / total
    fs[...] = jnp.transpose(fs[...])

    def block_of(side, k):
        return lax.rem(x + k, nx) if side == 0 else nx + lax.rem(y + k, ny)

    def near(side, k):
        return on_x(k) if side == 0 else on_y(k)

    def far(side, k):
        return on_y(k) if side == 0 else on_x(k)

    def order_of(side):
        return y if side == 0 else x

    cols = [fs[pl.ds(x * per + j, 8, stride=PAD), :] for j in range(per)]
    one, two, three, four, last = {}, {}, {}, {}, {c: [] for c in range(nc)}
    for c in range(nc):
        for cp in parts[c]:
            cp.wait_recv()
        for j in range(per):
            rows = []
            for g in range(step // 8):
                lead = c * (step // 8) + g
                acc = cols[j][:, lead:lead + 1] * acch[x * per + j, pl.ds(half * p + 8 * lead, 8)]
                for i in range(1, ns):
                    acc = acc + cols[j][:, i * n8 + lead:i * n8 + lead + 1] * rx[i, c, j, 8 * g:8 * g + 8]
                rows.append(acc)
            lhs[c, :, j * dim:(j + 1) * dim] = jnp.concatenate(rows, axis=0).astype(BF16)
        if c == 0:
            load.wait()
            wcopy.wait_recv()
        for k in (2, 1, 3, 0):
            for side in range(2):
                n = block_of(side, k)
                z[c, side * 4 + k] = jnp.dot(lhs[c], wob[:, pl.ds(pl.multiple_of(n * wide, wide), wide)],
                                             preferred_element_type=F32)
            for side in range(2 if k else 0):
                i = side * 4 + k
                one[c, side, k] = go(z.at[c, i], r1.at[c, i], a_s.at[c, i], a_r.at[c, i], near(side, k))

    for c in range(nc):
        for side in range(2):
            base = side * 4
            for k in (1, 3, 2):
                one[c, side, k].wait_recv()
            v = z[c, base] + r1[c, base + 1] + r1[c, base + 2] + r1[c, base + 3]
            for r in range(4):
                s1[c, side, r] = v[8 * (r // 2):8 * (r // 2) + 8, short * (r % 2):short * (r % 2 + 1)]
            for k in (2, 1, 3):
                dest = lax.rem(order_of(side) + k, 4)
                i = base + k
                two[c, side, k] = go(s1.at[c, side, dest], r2.at[c, i], b_s.at[c, i], b_r.at[c, i], far(side, k))

    for c in range(nc):
        for side in range(2):
            base = side * 4
            for k in (1, 3, 2):
                two[c, side, k].wait_recv()
            v = s1[c, side, order_of(side)] + r2[c, base + 1] + r2[c, base + 2] + r2[c, base + 3]
            part = yb.at[block_of(side, 0), p, c, order_of(side)]
            part[...] = v.astype(BF16)
            for k in (2, 1, 3):
                i = base + k
                three[c, side, k] = go(part, part, c_s.at[c, i], c_r.at[c, i], far(side, k))

    def mirror(c, side, k):
        part = yb.at[block_of(side, 4 - k), p, c]
        i = side * 4 + k
        last[c].append(go(part, part, f_s.at[c, i], f_r.at[c, i], partner))

    for c in range(nc):
        for side in range(2):
            part = yb.at[block_of(side, 0), p, c]
            for k in (1, 3, 2):
                three[c, side, k].wait_recv()
            for k in (2, 1, 3):
                i = side * 4 + k
                four[c, side, k] = go(part, part, e_s.at[c, i], e_r.at[c, i], near(side, k))
            mirror(c, side, 0)
    for c in range(nc):
        for k in (1, 3, 2):
            for side in range(2):
                four[c, side, k].wait_recv()
                mirror(c, side, k)
    for c in range(nc):
        for cp in last[c]:
            cp.wait_recv()
        for n in range(2 * nx):
            for q in range(2):
                for r in range(4):
                    row = q * 4 + c * 2 + r // 2
                    left = n * wide + (r % 2) * short
                    out[row, :, left:left + short] = yb[n, q, c, r]
    for cp in sends:
        cp.wait_send()


def solution(mesh):
    cache_spec = P('rep', 'seq', 'head', None)

    def local_step(tokens, w_query, w_key, w_value, w_out, k_cache, v_cache, positions):
        batch, shard, kv, dim = k_cache.shape
        model = tokens.shape[1]
        groups = w_query.shape[1] // w_key.shape[1]
        heads = kv * groups
        rows = shard * kv
        flat = (batch, rows, dim)
        hspec = pl.BlockSpec(memory_space=pltpu.HBM)
        anyspec = pl.BlockSpec(memory_space=pl.ANY)
        vspec = pl.BlockSpec(memory_space=pltpu.VMEM)
        dma = pltpu.SemaphoreType.DMA
        cache = jax.ShapeDtypeStruct(flat, BF16)
        blocks = groups + 2
        proj, kb, vb = pl.pallas_call(
            functools.partial(project, groups),
            out_shape=(jax.ShapeDtypeStruct((blocks, batch, kv * dim), BF16), cache, cache),
            in_specs=[hspec] * 6,
            out_specs=(vspec,) * 3,
            scratch_shapes=[pltpu.VMEM(tokens.shape, BF16), pltpu.VMEM((4, model // 4, kv * dim), BF16), dma,
                            dma((4,)), dma((8,)), dma((8,)), dma, dma],
            compiler_params=pltpu.CompilerParams(collective_id=1, has_side_effects=True, vmem_limit_bytes=34 << 20),
            cost_estimate=pl.CostEstimate(flops=10**10, bytes_accessed=30 * 10**6, transcendentals=0),
            name='project',
        )(tokens, w_query, w_key, w_value, k_cache.reshape(flat), v_cache.reshape(flat))
        k_new, v_new, _, _, acc, stat = pl.pallas_call(
            functools.partial(attend, groups),
            out_shape=(cache, cache, cache, cache, jax.ShapeDtypeStruct((heads, batch, dim), F32),
                       jax.ShapeDtypeStruct((PAD, dim), F32)),
            in_specs=[vspec, vspec, vspec, pl.BlockSpec(memory_space=pltpu.SMEM)],
            out_specs=(hspec, hspec, vspec, vspec, vspec, vspec),
            input_output_aliases={1: 2, 2: 3},
            scratch_shapes=[pltpu.VMEM((batch * PAD, dim), F32), pltpu.VMEM((2, batch, kv * dim), F32),
                            pltpu.VMEM((batch * PAD, dim), F32), pltpu.VMEM((2, rows, NB * PAD), F32),
                            dma((2, batch // NB))],
            compiler_params=pltpu.CompilerParams(vmem_limit_bytes=24 << 20),
            cost_estimate=pl.CostEstimate(flops=10**10, bytes_accessed=17 * 10**6, transcendentals=0),
            name='attend',
        )(proj, kb, vb, positions)

        wide = model // 8
        step = batch // 2 // NC
        ns = lax.axis_size('seq')
        y = pl.pallas_call(
            finish,
            out_shape=jax.ShapeDtypeStruct((8, 8, model), BF16),
            in_specs=[vspec, vspec, anyspec],
            out_specs=vspec,
            scratch_shapes=[
                pltpu.VMEM((2 * w_out.shape[0], model), BF16),
                pltpu.VMEM((ns, NC, 2 * heads // ns, step, dim), F32),
                pltpu.VMEM((ns, 8, dim), F32),
                pltpu.VMEM((dim, dim), F32),
                pltpu.VMEM((NC, step, 2 * w_out.shape[0]), BF16),
                pltpu.VMEM((NC, 8, step, wide), F32),
                pltpu.VMEM((NC, 8, step, wide), F32),
                pltpu.VMEM((NC, 2, 4, 8, wide // 2), F32),
                pltpu.VMEM((NC, 8, 8, wide // 2), F32),
                pltpu.VMEM((8, 2, NC, 4, 8, wide // 2), BF16),
                dma, dma, dma,
                dma((NC, 8)), dma((NC, 8)), dma((8,)), dma((8,)),
            ] + [dma((NC, 8))] * 10,
            compiler_params=pltpu.CompilerParams(collective_id=0, has_side_effects=True, vmem_limit_bytes=32 << 20),
            name='finish',
        )(acc, stat, w_out)
        return y.reshape(batch, model), k_new.reshape(k_cache.shape), v_new.reshape(v_cache.shape)

    return jax.shard_map(
        local_step,
        mesh=mesh,
        in_specs=(P('rep', None), P(), P(), P(), P(('head', 'seq'), None), cache_spec, cache_spec, P('rep')),
        out_specs=(P('rep', None), cache_spec, cache_spec),
        check_vma=False,
    )
```

```python
import functools

import jax
import jax.numpy as jnp
from jax import lax
from jax.experimental import pallas as pl
from jax.experimental.pallas import tpu as pltpu
from jax.sharding import PartitionSpec as P

MESH = pl.DeviceIdType.MESH
BF16 = jnp.bfloat16
F32 = jnp.float32
PAD = 16
NB = 16
NC = 2


def project(groups, tokens, wq, wk, wv, kc, vc, pj, kb, vb, tok, wbuf, tsem, wsem, ssem, rsem, ksem, vsem):
    head = lax.axis_index('head')
    s = lax.axis_index('seq')
    ns = lax.axis_size('seq')
    parts, depth, width = wbuf.shape

    def load(i, src, block):
        rows = pl.ds(i * depth, depth)
        return pltpu.make_async_copy(src.at[rows, pl.ds(pl.multiple_of(block * width, width), width)], wbuf.at[i], wsem.at[i])

    first = pltpu.make_async_copy(tokens, tok, tsem)
    first.start()
    for i in range(parts):
        @pl.when(s < groups)
        def _():
            load(i, wq, head * groups + s).start()

        @pl.when(s == groups)
        def _():
            load(i, wk, head).start()

        @pl.when(s == groups + 1)
        def _():
            load(i, wv, head).start()

    caches = [pltpu.make_async_copy(kc, kb, ksem), pltpu.make_async_copy(vc, vb, vsem)]
    for cp in caches:
        cp.start()
    barrier = pltpu.get_barrier_semaphore()
    for k in range(1, ns):
        pl.semaphore_signal(barrier, inc=1, device_id={'head': head, 'seq': lax.rem(s + k, ns)}, device_id_type=MESH)
    first.wait()
    acc = jnp.zeros((tok.shape[0], width), F32)
    for i in range(parts):
        load(i, wq, 0).wait()
        acc = acc + jnp.dot(tok[:, i * depth:(i + 1) * depth], wbuf[i], preferred_element_type=F32)
    pj[s] = acc.astype(BF16)
    pl.semaphore_wait(barrier, ns - 1)
    sends = []
    for k in (4, 5, 3, 2, 6, 7, 1):
        cp = pltpu.make_async_remote_copy(src_ref=pj.at[s], dst_ref=pj.at[s], send_sem=ssem.at[k], recv_sem=rsem.at[k],
                                          device_id={'head': head, 'seq': lax.rem(s + k, ns)}, device_id_type=MESH)
        cp.start()
        sends.append(cp)
    for cp in sends:
        cp.wait_recv()
    for cp in sends:
        cp.wait_send()
    for cp in caches:
        cp.wait()


def attend(groups, pj, kin, vin, pos, ko, vo, kb, vb, acch, stat, q2, nkv, accs, sb, osem):
    seq = lax.axis_index('seq')
    batch, rows, dim = kb.shape
    shard = rows // 2
    heads = 2 * groups
    steps = batch // NB
    nkv[0] = pj[groups].astype(F32)
    nkv[1] = pj[groups + 1].astype(F32)

    row16 = lax.broadcasted_iota(jnp.int32, (16, dim), 0)
    even = (row16 & 1) == 0
    lanes = NB * PAD
    lane = lax.broadcasted_iota(jnp.int32, (8, lanes), 1)
    sub = lax.broadcasted_iota(jnp.int32, (8, lanes), 0)
    hl = lane & (PAD - 1)
    match = jnp.where(hl < groups, 0, jnp.where(hl < heads, 1, 2)) == (sub & 1)
    tile = lax.broadcasted_iota(jnp.int32, (rows // 8, 8, lanes), 0) * 4

    def out(j, c):
        span = pl.ds(pl.multiple_of(c * NB, NB), NB)
        src, dst = ((kb, ko), (vb, vo))[j]
        return pltpu.make_async_copy(src.at[span], dst.at[span], osem.at[j, c])

    def refresh(c, carry):
        fresh = []
        for i in range(NB):
            b = c * NB + i
            t = pos[b] - seq * shard
            inside = (t >= 0) & (t < shard)
            tc = jnp.clip(t, 0, shard - 1)
            start = pl.multiple_of((tc >> 3) * 16, 16)
            hit = ((row16 >> 1) == (tc & 7)) & inside
            for j, buf in enumerate((kb, vb)):
                new = nkv[j, pl.ds(b, 1), :]
                new = jnp.where(even, new[:, :dim], new[:, dim:])
                old = buf[b, pl.ds(start, 16), :].astype(F32)
                fresh.append((buf, b, start, jnp.where(hit, new, old).astype(BF16)))
        for buf, b, start, value in fresh:
            buf[b, pl.ds(start, 16), :] = value
        out(0, c).start()
        out(1, c).start()
        return carry

    lax.fori_loop(0, steps, refresh, 0)
    q2[...] = jnp.zeros_like(q2)
    for h in range(heads):
        q2[pl.ds(h, batch, stride=PAD), :] = pj[h // 2][:, (h % 2) * dim:(h % 2 + 1) * dim].astype(F32)
    ql = lax.broadcasted_iota(jnp.int32, (dim, lanes), 1) // PAD

    def scores(c):
        qt = jnp.transpose(q2[c * lanes:(c + 1) * lanes, :]).astype(BF16)
        zero = jnp.zeros_like(qt)
        s = jnp.zeros((rows, lanes), F32)
        for j in range(NB // 2):
            b = c * NB + 2 * j
            lhs = jnp.concatenate([kb[b], kb[b + 1]], axis=1)
            rhs = jnp.concatenate([jnp.where(ql == 2 * j, qt, zero), jnp.where(ql == 2 * j + 1, qt, zero)], axis=0)
            s = s + jnp.dot(lhs, rhs, preferred_element_type=F32)
        sb[c % 2] = s

    def mix(c):
        limit = jnp.zeros((8, lanes), jnp.int32)
        for i in range(NB):
            limit = jnp.where(lane // PAD == i, pos[c * NB + i] - seq * shard, limit)
        edge = jnp.where(match, limit, -1) - (sub >> 1)
        s = sb[c % 2].reshape(rows // 8, 8, lanes) * dim ** -0.5
        s = jnp.where(tile <= edge[None], s, -jnp.inf)
        m = jnp.max(jnp.max(s, axis=0), axis=0, keepdims=True)
        w = jnp.exp(s - jnp.where(m == -jnp.inf, 0.0, m)[None])
        l = jnp.sum(jnp.sum(w, axis=0), axis=0, keepdims=True)
        for r in range(lanes // dim):
            g = c * (lanes // dim) + r
            g = g // 4 * 8 + g % 4
            stat[g:g + 1, :] = m[:, r * dim:(r + 1) * dim]
            stat[g + 4:g + 5, :] = l[:, r * dim:(r + 1) * dim]
        wt = jnp.transpose(w.reshape(rows, lanes).astype(BF16))
        for j in range(NB // 2):
            b = c * NB + 2 * j
            rhs = jnp.concatenate([vb[b], vb[b + 1]], axis=1)
            a = jnp.dot(wt[2 * PAD * j:2 * PAD * (j + 1)], rhs, preferred_element_type=F32)
            accs[b * PAD:(b + 1) * PAD, :] = a[:PAD, :dim]
            accs[(b + 1) * PAD:(b + 2) * PAD, :] = a[PAD:, dim:]

    scores(0)
    for c in range(steps):
        if c + 1 < steps:
            scores(c + 1)
        mix(c)
    for h in range(heads):
        acch[h] = accs[pl.ds(h, batch, stride=PAD), :]
    for c in range(steps):
        out(0, c).wait()
        out(1, c).wait()


def finish(acch, stat, wo, out, wob, rx, srx, fs, lhs, z, r1, s1, r2,
           osem, w_s, w_r, d_s, d_r, t_s, t_r, a_s, a_r, b_s, b_r, c_s, c_r, e_s, e_r, f_s, f_r):
    y = lax.axis_index('head')
    s = lax.axis_index('seq')
    ny = lax.axis_size('head')
    ns = lax.axis_size('seq')
    nx = ns // 2
    x = s // 2
    p = lax.rem(s, 2)
    heads, batch, dim = acch.shape
    wrows = wo.shape[0]
    nc, per, step = rx.shape[1:4]
    half = nc * step
    wide = z.shape[-1]
    short = wide // 2

    def on_x(k):
        return {'head': y, 'seq': lax.rem(x + k, nx) * 2 + p}

    def on_y(k):
        return {'head': lax.rem(y + k, ny), 'seq': s}

    def copy(src, dst, send, recv, dev):
        return pltpu.make_async_remote_copy(src_ref=src, dst_ref=dst, send_sem=send, recv_sem=recv,
                                            device_id=dev, device_id_type=MESH)

    partner = {'head': y, 'seq': x * 2 + 1 - p}
    mine = wob.at[pl.ds(pl.multiple_of(p * wrows, wrows), wrows), :]
    load = pltpu.make_async_copy(wo, mine, osem)
    load.start()

    barrier = pltpu.get_barrier_semaphore()
    for k in range(1, ns):
        pl.semaphore_signal(barrier, inc=1, device_id={'head': y, 'seq': lax.rem(s + k, ns)}, device_id_type=MESH)
    for k in range(1, ny):
        pl.semaphore_signal(barrier, inc=1, device_id=on_y(k), device_id_type=MESH)
    pl.semaphore_wait(barrier, ns - 1 + ny - 1)

    sends = []

    def go(*a):
        cp = copy(*a)
        cp.start()
        sends.append(cp)
        return cp

    def flush(n):
        for cp in sends[:n]:
            cp.wait_send()
        del sends[:n]

    stats, parts = [], {c: [] for c in range(nc)}
    for c in range(nc):
        for k in (4, 5, 3, 2, 6, 7, 1):
            dest = lax.rem(s + k, ns)
            dev = {'head': y, 'seq': dest}
            side = lax.rem(dest, 2)
            if c == 0:
                rows = pl.ds(pl.multiple_of(side * 8, 8), 8)
                stats.append(go(stat.at[rows], srx.at[k], t_s.at[k], t_r.at[k], dev))
            rows = pl.ds(pl.multiple_of(side * half + c * step, step), step)
            parts[c].append(go(acch.at[pl.ds((dest // 2) * per, per), rows], rx.at[k, c], d_s.at[c, k], d_r.at[c, k], dev))
    wcopy = go(wo, mine, w_s, w_r, partner)
    srx[0] = stat[pl.ds(pl.multiple_of(p * 8, 8), 8)]
    fs[...] = jnp.zeros_like(fs)
    for cp in stats:
        cp.wait_recv()
    n8 = half // 8
    top = functools.reduce(jnp.maximum, [srx[i, :n8] for i in range(ns)])
    scale = [jnp.exp(srx[i, :n8] - top) for i in range(ns)]
    total = functools.reduce(lambda a, b: a + b, [e * srx[i, n8:] for i, e in enumerate(scale)])
    for i in range(ns):
        fs[i * n8:(i + 1) * n8, :] = scale[i] / total
    fs[...] = jnp.transpose(fs[...])

    def block_of(side, k):
        return lax.rem(x + k, nx) if side == 0 else nx + lax.rem(y + k, ny)

    def near(side, k):
        return on_x(k) if side == 0 else on_y(k)

    def far(side, k):
        return on_y(k) if side == 0 else on_x(k)

    def order_of(side):
        return y if side == 0 else x

    early = len(sends)
    cols = [fs[pl.ds(x * per + j, 8, stride=PAD), :] for j in range(per)]
    one, two, three, four, last = {}, {}, {}, {}, {c: [] for c in range(nc)}
    for c in range(nc):
        for cp in parts[c]:
            cp.wait_recv()
        for j in range(per):
            rows = []
            for g in range(step // 8):
                lead = c * (step // 8) + g
                acc = cols[j][:, lead:lead + 1] * acch[x * per + j, pl.ds(half * p + 8 * lead, 8)]
                for i in range(1, ns):
                    acc = acc + cols[j][:, i * n8 + lead:i * n8 + lead + 1] * rx[i, c, j, 8 * g:8 * g + 8]
                rows.append(acc)
            lhs[c, :, j * dim:(j + 1) * dim] = jnp.concatenate(rows, axis=0).astype(BF16)
        if c == 0:
            load.wait()
            wcopy.wait_recv()
        for k in (2, 1, 3, 0):
            for side in range(2):
                n = block_of(side, k)
                z[c, side * 4 + k] = jnp.dot(lhs[c], wob[:, pl.ds(pl.multiple_of(n * wide, wide), wide)],
                                             preferred_element_type=F32)
            for side in range(2 if k else 0):
                i = side * 4 + k
                one[c, side, k] = go(z.at[c, i], r1.at[c, i], a_s.at[c, i], a_r.at[c, i], near(side, k))

    for c in range(nc):
        for side in range(2):
            base = side * 4
            for k in (1, 3, 2):
                one[c, side, k].wait_recv()
            v = z[c, base] + r1[c, base + 1] + r1[c, base + 2] + r1[c, base + 3]
            for r in range(4):
                s1[c, side, r] = v[8 * (r // 2):8 * (r // 2) + 8, short * (r % 2):short * (r % 2 + 1)]
            for k in (2, 1, 3):
                dest = lax.rem(order_of(side) + k, 4)
                i = base + k
                two[c, side, k] = go(s1.at[c, side, dest], r2.at[c, i], b_s.at[c, i], b_r.at[c, i], far(side, k))

    flush(early)

    def piece(c, n, r=None):
        row = 4 * p + 2 * c
        if r is None:
            return out.at[pl.ds(row, 2), :, pl.ds(pl.multiple_of(n * wide, wide), wide)]
        return out.at[row + r // 2, :, pl.ds(pl.multiple_of(n * wide + lax.rem(r, 2) * short, short), short)]

    for c in range(nc):
        for side in range(2):
            base = side * 4
            for k in (1, 3, 2):
                two[c, side, k].wait_recv()
            v = s1[c, side, order_of(side)] + r2[c, base + 1] + r2[c, base + 2] + r2[c, base + 3]
            part = piece(c, block_of(side, 0), order_of(side))
            part[...] = v.astype(BF16)
            for k in (2, 1, 3):
                i = base + k
                three[c, side, k] = go(part, part, c_s.at[c, i], c_r.at[c, i], far(side, k))

    flush(6 * nc)

    def mirror(c, side, k):
        part = piece(c, block_of(side, 4 - k))
        i = side * 4 + k
        last[c].append(go(part, part, f_s.at[c, i], f_r.at[c, i], partner))

    for c in range(nc):
        for side in range(2):
            part = piece(c, block_of(side, 0))
            for k in (1, 3, 2):
                three[c, side, k].wait_recv()
            for k in (2, 1, 3):
                i = side * 4 + k
                four[c, side, k] = go(part, part, e_s.at[c, i], e_r.at[c, i], near(side, k))
            mirror(c, side, 0)
    flush(6 * nc)
    for c in range(nc):
        for k in (1, 3, 2):
            for side in range(2):
                four[c, side, k].wait_recv()
                mirror(c, side, k)
    flush(6 * nc)
    for c in range(nc):
        for cp in last[c]:
            cp.wait_recv()
    for cp in sends:
        cp.wait_send()


def solution(mesh):
    cache_spec = P('rep', 'seq', 'head', None)

    def local_step(tokens, w_query, w_key, w_value, w_out, k_cache, v_cache, positions):
        batch, shard, kv, dim = k_cache.shape
        model = tokens.shape[1]
        groups = w_query.shape[1] // w_key.shape[1]
        heads = kv * groups
        rows = shard * kv
        flat = (batch, rows, dim)
        hspec = pl.BlockSpec(memory_space=pltpu.HBM)
        anyspec = pl.BlockSpec(memory_space=pl.ANY)
        vspec = pl.BlockSpec(memory_space=pltpu.VMEM)
        dma = pltpu.SemaphoreType.DMA
        cache = jax.ShapeDtypeStruct(flat, BF16)
        blocks = groups + 2
        proj, kb, vb = pl.pallas_call(
            functools.partial(project, groups),
            out_shape=(jax.ShapeDtypeStruct((blocks, batch, kv * dim), BF16), cache, cache),
            in_specs=[hspec] * 6,
            out_specs=(vspec,) * 3,
            scratch_shapes=[pltpu.VMEM(tokens.shape, BF16), pltpu.VMEM((4, model // 4, kv * dim), BF16), dma,
                            dma((4,)), dma((8,)), dma((8,)), dma, dma],
            compiler_params=pltpu.CompilerParams(collective_id=1, has_side_effects=True, vmem_limit_bytes=16 << 20),
            cost_estimate=pl.CostEstimate(flops=10**10, bytes_accessed=30 * 10**6, transcendentals=0),
            name='project',
        )(*[pltpu.with_memory_space_constraint(a, pltpu.HBM) for a in (
            tokens, w_query, w_key, w_value, k_cache.reshape(flat), v_cache.reshape(flat))])
        k_new, v_new, _, _, acc, stat = pl.pallas_call(
            functools.partial(attend, groups),
            out_shape=(cache, cache, cache, cache, jax.ShapeDtypeStruct((heads, batch, dim), F32),
                       jax.ShapeDtypeStruct((PAD, dim), F32)),
            in_specs=[vspec, vspec, vspec, pl.BlockSpec(memory_space=pltpu.SMEM)],
            out_specs=(hspec, hspec, vspec, vspec, vspec, vspec),
            input_output_aliases={1: 2, 2: 3},
            scratch_shapes=[pltpu.VMEM((batch * PAD, dim), F32), pltpu.VMEM((2, batch, kv * dim), F32),
                            pltpu.VMEM((batch * PAD, dim), F32), pltpu.VMEM((2, rows, NB * PAD), F32),
                            dma((2, batch // NB))],
            compiler_params=pltpu.CompilerParams(vmem_limit_bytes=12 << 20),
            cost_estimate=pl.CostEstimate(flops=10**10, bytes_accessed=17 * 10**6, transcendentals=0),
            name='attend',
        )(proj, kb, vb, positions)

        wide = model // 8
        step = batch // 2 // NC
        ns = lax.axis_size('seq')
        y = pl.pallas_call(
            finish,
            out_shape=jax.ShapeDtypeStruct((8, 8, model), BF16),
            in_specs=[vspec, vspec, anyspec],
            out_specs=vspec,
            scratch_shapes=[
                pltpu.VMEM((2 * w_out.shape[0], model), BF16),
                pltpu.VMEM((ns, NC, 2 * heads // ns, step, dim), F32),
                pltpu.VMEM((ns, 8, dim), F32),
                pltpu.VMEM((dim, dim), F32),
                pltpu.VMEM((NC, step, 2 * w_out.shape[0]), BF16),
                pltpu.VMEM((NC, 8, step, wide), F32),
                pltpu.VMEM((NC, 8, step, wide), F32),
                pltpu.VMEM((NC, 2, 4, 8, wide // 2), F32),
                pltpu.VMEM((NC, 8, 8, wide // 2), F32),
                dma, dma, dma,
                dma((NC, 8)), dma((NC, 8)), dma((8,)), dma((8,)),
            ] + [dma((NC, 8))] * 10,
            compiler_params=pltpu.CompilerParams(collective_id=0, has_side_effects=True, vmem_limit_bytes=32 << 20),
            name='finish',
        )(acc, stat, w_out)
        return y.reshape(batch, model), k_new.reshape(k_cache.shape), v_new.reshape(v_cache.shape)

    return jax.shard_map(
        local_step,
        mesh=mesh,
        in_specs=(P('rep', None), P(), P(), P(), P(('head', 'seq'), None), cache_spec, cache_spec, P('rep')),
        out_specs=(P('rep', None), cache_spec, cache_spec),
        check_vma=False,
    )
```

```python
import functools

import jax
import jax.numpy as jnp
from jax import lax
from jax.experimental import pallas as pl
from jax.experimental.pallas import tpu as pltpu
from jax.sharding import PartitionSpec as P

MESH = pl.DeviceIdType.MESH
BF16 = jnp.bfloat16
F32 = jnp.float32
PAD = 16
NB = 16
NR = 8
NC = 2


def project(groups, tokens, wq, wk, wv, kc, vc, pj, kb, vb, tok, wbuf, tsem, wsem, ssem, rsem, ksem, vsem):
    head = lax.axis_index('head')
    s = lax.axis_index('seq')
    ns = lax.axis_size('seq')
    parts, depth, width = wbuf.shape

    def load(i, src, block):
        rows = pl.ds(i * depth, depth)
        return pltpu.make_async_copy(src.at[rows, pl.ds(pl.multiple_of(block * width, width), width)], wbuf.at[i], wsem.at[i])

    first = pltpu.make_async_copy(tokens, tok, tsem)
    first.start()
    for i in range(parts):
        @pl.when(s < groups)
        def _():
            load(i, wq, head * groups + s).start()

        @pl.when(s == groups)
        def _():
            load(i, wk, head).start()

        @pl.when(s == groups + 1)
        def _():
            load(i, wv, head).start()

    caches = [pltpu.make_async_copy(kc, kb, ksem), pltpu.make_async_copy(vc, vb, vsem)]
    for cp in caches:
        cp.start()
    barrier = pltpu.get_barrier_semaphore()
    for k in range(1, ns):
        pl.semaphore_signal(barrier, inc=1, device_id={'head': head, 'seq': lax.rem(s + k, ns)}, device_id_type=MESH)
    first.wait()
    acc = jnp.zeros((tok.shape[0], width), F32)
    for i in range(parts):
        load(i, wq, 0).wait()
        acc = acc + jnp.dot(tok[:, i * depth:(i + 1) * depth], wbuf[i], preferred_element_type=F32)
    pj[s] = acc.astype(BF16)
    pl.semaphore_wait(barrier, ns - 1)
    sends = []
    for k in (4, 5, 3, 2, 6, 7, 1):
        cp = pltpu.make_async_remote_copy(src_ref=pj.at[s], dst_ref=pj.at[s], send_sem=ssem.at[k], recv_sem=rsem.at[k],
                                          device_id={'head': head, 'seq': lax.rem(s + k, ns)}, device_id_type=MESH)
        cp.start()
        sends.append(cp)
    for cp in sends:
        cp.wait_recv()
    for cp in sends:
        cp.wait_send()
    for cp in caches:
        cp.wait()


def attend(groups, pj, kin, vin, pos, ko, vo, kb, vb, acch, stat, q2, nkv, accs, sb, osem):
    seq = lax.axis_index('seq')
    batch, rows, dim = kb.shape
    shard = rows // 2
    heads = 2 * groups
    steps = batch // NB
    nkv[0] = pj[groups].astype(F32)
    nkv[1] = pj[groups + 1].astype(F32)

    row16 = lax.broadcasted_iota(jnp.int32, (16, dim), 0)
    even = (row16 & 1) == 0
    lanes = NB * PAD
    lane = lax.broadcasted_iota(jnp.int32, (8, lanes), 1)
    sub = lax.broadcasted_iota(jnp.int32, (8, lanes), 0)
    hl = lane & (PAD - 1)
    match = jnp.where(hl < groups, 0, jnp.where(hl < heads, 1, 2)) == (sub & 1)
    tile = lax.broadcasted_iota(jnp.int32, (rows // 8, 8, lanes), 0) * 4

    def out(j, c):
        span = pl.ds(pl.multiple_of(c * NR, NR), NR)
        src, dst = ((kb, ko), (vb, vo))[j]
        return pltpu.make_async_copy(src.at[span], dst.at[span], osem.at[j, c])

    def refresh(c, carry):
        fresh = []
        for i in range(NR):
            b = c * NR + i
            t = pos[b] - seq * shard
            inside = (t >= 0) & (t < shard)
            tc = jnp.clip(t, 0, shard - 1)
            start = pl.multiple_of((tc >> 3) * 16, 16)
            hit = ((row16 >> 1) == (tc & 7)) & inside
            for j, buf in enumerate((kb, vb)):
                new = nkv[j, pl.ds(b, 1), :]
                new = jnp.where(even, new[:, :dim], new[:, dim:])
                old = buf[b, pl.ds(start, 16), :].astype(F32)
                fresh.append((buf, b, start, jnp.where(hit, new, old).astype(BF16)))
        for buf, b, start, value in fresh:
            buf[b, pl.ds(start, 16), :] = value
        out(0, c).start()
        out(1, c).start()
        return carry

    lax.fori_loop(0, batch // NR, refresh, 0)
    q2[...] = jnp.zeros_like(q2)
    for h in range(heads):
        q2[pl.ds(h, batch, stride=PAD), :] = pj[h // 2][:, (h % 2) * dim:(h % 2 + 1) * dim].astype(F32)
    ql = lax.broadcasted_iota(jnp.int32, (dim, lanes), 1) // PAD

    def scores(c):
        qt = jnp.transpose(q2[c * lanes:(c + 1) * lanes, :]).astype(BF16)
        zero = jnp.zeros_like(qt)
        s = jnp.zeros((rows, lanes), F32)
        for j in range(NB // 2):
            b = c * NB + 2 * j
            lhs = jnp.concatenate([kb[b], kb[b + 1]], axis=1)
            rhs = jnp.concatenate([jnp.where(ql == 2 * j, qt, zero), jnp.where(ql == 2 * j + 1, qt, zero)], axis=0)
            s = s + jnp.dot(lhs, rhs, preferred_element_type=F32)
        sb[c % 2] = s

    def mix(c):
        limit = jnp.zeros((8, lanes), jnp.int32)
        for i in range(NB):
            limit = jnp.where(lane // PAD == i, pos[c * NB + i] - seq * shard, limit)
        edge = jnp.where(match, limit, -1) - (sub >> 1)
        s = sb[c % 2].reshape(rows // 8, 8, lanes) * dim ** -0.5
        s = jnp.where(tile <= edge[None], s, -jnp.inf)
        m = jnp.max(jnp.max(s, axis=0), axis=0, keepdims=True)
        w = jnp.exp(s - jnp.where(m == -jnp.inf, 0.0, m)[None])
        l = jnp.sum(jnp.sum(w, axis=0), axis=0, keepdims=True)
        for r in range(lanes // dim):
            g = c * (lanes // dim) + r
            g = g // 4 * 8 + g % 4
            stat[g:g + 1, :] = m[:, r * dim:(r + 1) * dim]
            stat[g + 4:g + 5, :] = l[:, r * dim:(r + 1) * dim]
        wt = jnp.transpose(w.reshape(rows, lanes).astype(BF16))
        for j in range(NB // 2):
            b = c * NB + 2 * j
            rhs = jnp.concatenate([vb[b], vb[b + 1]], axis=1)
            a = jnp.dot(wt[2 * PAD * j:2 * PAD * (j + 1)], rhs, preferred_element_type=F32)
            accs[b * PAD:(b + 1) * PAD, :] = a[:PAD, :dim]
            accs[(b + 1) * PAD:(b + 2) * PAD, :] = a[PAD:, dim:]

    scores(0)
    for c in range(steps):
        if c + 1 < steps:
            scores(c + 1)
        mix(c)
    for h in range(heads):
        acch[h] = accs[pl.ds(h, batch, stride=PAD), :]
    for c in range(batch // NR):
        out(0, c).wait()
        out(1, c).wait()


def finish(acch, stat, wo, out, wob, rx, srx, sx, dx, pr, fs, lhs, z, r1, s1, r2,
           osem, w_s, w_r, d_s, d_r, t_s, t_r, a_s, a_r, b_s, b_r, c_s, c_r, e_s, e_r, f_s, f_r):
    y = lax.axis_index('head')
    s = lax.axis_index('seq')
    ny = lax.axis_size('head')
    ns = lax.axis_size('seq')
    nx = ns // 2
    x = s // 2
    p = lax.rem(s, 2)
    heads, batch, dim = acch.shape
    wrows = wo.shape[0]
    nc, per, step = rx.shape[1:4]
    half = nc * step
    wide = z.shape[-1]
    short = wide // 2

    def on_x(k):
        return {'head': y, 'seq': lax.rem(x + k, nx) * 2 + p}

    def on_y(k):
        return {'head': lax.rem(y + k, ny), 'seq': s}

    def copy(src, dst, send, recv, dev):
        return pltpu.make_async_remote_copy(src_ref=src, dst_ref=dst, send_sem=send, recv_sem=recv,
                                            device_id=dev, device_id_type=MESH)

    partner = {'head': y, 'seq': x * 2 + 1 - p}
    mine = wob.at[pl.ds(pl.multiple_of(p * wrows, wrows), wrows), :]
    load = pltpu.make_async_copy(wo, mine, osem)
    load.start()

    barrier = pltpu.get_barrier_semaphore()
    for k in (2, 1, 3):
        pl.semaphore_signal(barrier, inc=1, device_id=on_x(k), device_id_type=MESH)
        pl.semaphore_signal(barrier, inc=1, device_id=on_y(k), device_id_type=MESH)
    pl.semaphore_signal(barrier, inc=1, device_id=partner, device_id_type=MESH)
    pl.semaphore_wait(barrier, 7)

    sends = []

    def go(*a):
        cp = copy(*a)
        cp.start()
        sends.append(cp)
        return cp

    def flush(n):
        for cp in sends[:n]:
            cp.wait_send()
        del sends[:n]

    there, here = 1 - p, p
    scopy = go(stat.at[pl.ds(pl.multiple_of(there * 8, 8), 8)], sx, t_s.at[0], t_r.at[0], partner)
    pairs = []
    for c in range(nc):
        rows = pl.ds(pl.multiple_of(there * half + c * step, step), step)
        pairs.append(go(acch.at[:, rows], dx.at[c], d_s.at[c, 0], d_r.at[c, 0], partner))
    wcopy = go(wo, mine, w_s, w_r, partner)
    n8 = half // 8
    fs[...] = jnp.zeros_like(fs)
    ours = stat[pl.ds(pl.multiple_of(here * 8, 8), 8)]
    scopy.wait_recv()
    theirs = sx[...]
    peak = jnp.maximum(ours[:n8], theirs[:n8])
    base = jnp.where(peak == -jnp.inf, 0.0, peak)
    scale = [jnp.exp(t[:n8] - base) for t in (ours, theirs)]
    srx[0, :n8] = peak
    srx[0, n8:] = scale[0] * ours[n8:] + scale[1] * theirs[n8:]
    stats = [go(srx.at[0], srx.at[k], t_s.at[k], t_r.at[k], on_x(k)) for k in (2, 1, 3)]
    fs[:n8] = scale[0]
    fs[n8:2 * n8] = scale[1]
    fs[...] = jnp.transpose(fs[...])
    parts = {}
    for c in range(nc):
        pairs[c].wait_recv()
        for h in range(heads):
            col = fs[pl.ds(h, 8, stride=PAD), :]
            for g in range(step // 8):
                lead = c * (step // 8) + g
                pr[c, h, 8 * g:8 * g + 8] = (col[:, lead:lead + 1] * acch[h, pl.ds(half * here + 8 * lead, 8)]
                                             + col[:, n8 + lead:n8 + lead + 1] * dx[c, h, 8 * g:8 * g + 8])
        parts[c] = [go(pr.at[c, pl.ds(lax.rem(x + k, nx) * per, per)], rx.at[k, c], d_s.at[c, k], d_r.at[c, k], on_x(k))
                    for k in (2, 1, 3)]

    fs[...] = jnp.zeros_like(fs)
    for cp in stats:
        cp.wait_recv()
    top = functools.reduce(jnp.maximum, [srx[i, :n8] for i in range(nx)])
    scale = [jnp.exp(srx[i, :n8] - top) for i in range(nx)]
    total = functools.reduce(lambda a, b: a + b, [e * srx[i, n8:] for i, e in enumerate(scale)])
    for i in range(nx):
        fs[i * n8:(i + 1) * n8, :] = scale[i] / total
    fs[...] = jnp.transpose(fs[...])

    def block_of(side, k):
        return lax.rem(x + k, nx) if side == 0 else nx + lax.rem(y + k, ny)

    def near(side, k):
        return on_x(k) if side == 0 else on_y(k)

    def far(side, k):
        return on_y(k) if side == 0 else on_x(k)

    def order_of(side):
        return y if side == 0 else x

    early = len(sends)
    cols = [fs[pl.ds(x * per + j, 8, stride=PAD), :] for j in range(per)]
    one, two, three, four, last = {}, {}, {}, {}, {c: [] for c in range(nc)}
    for c in range(nc):
        for cp in parts[c]:
            cp.wait_recv()
        for j in range(per):
            rows = []
            for g in range(step // 8):
                lead = c * (step // 8) + g
                acc = cols[j][:, lead:lead + 1] * pr[c, x * per + j, 8 * g:8 * g + 8]
                for i in range(1, nx):
                    acc = acc + cols[j][:, i * n8 + lead:i * n8 + lead + 1] * rx[i, c, j, 8 * g:8 * g + 8]
                rows.append(acc)
            lhs[c, :, j * dim:(j + 1) * dim] = jnp.concatenate(rows, axis=0).astype(BF16)
        if c == 0:
            load.wait()
            wcopy.wait_recv()
        for k in (2, 1, 3, 0):
            for side in range(2):
                n = block_of(side, k)
                z[c, side * 4 + k] = jnp.dot(lhs[c], wob[:, pl.ds(pl.multiple_of(n * wide, wide), wide)],
                                             preferred_element_type=F32)
            for side in range(2 if k else 0):
                i = side * 4 + k
                one[c, side, k] = go(z.at[c, i], r1.at[c, i], a_s.at[c, i], a_r.at[c, i], near(side, k))

    for c in range(nc):
        for side in range(2):
            base = side * 4
            for k in (1, 3, 2):
                one[c, side, k].wait_recv()
            v = z[c, base] + r1[c, base + 1] + r1[c, base + 2] + r1[c, base + 3]
            for r in range(4):
                s1[c, side, r] = v[8 * (r // 2):8 * (r // 2) + 8, short * (r % 2):short * (r % 2 + 1)]
            for k in (2, 1, 3):
                dest = lax.rem(order_of(side) + k, 4)
                i = base + k
                two[c, side, k] = go(s1.at[c, side, dest], r2.at[c, i], b_s.at[c, i], b_r.at[c, i], far(side, k))

    flush(early)

    def piece(c, n, r=None):
        row = 4 * p + 2 * c
        if r is None:
            return out.at[pl.ds(row, 2), :, pl.ds(pl.multiple_of(n * wide, wide), wide)]
        return out.at[row + r // 2, :, pl.ds(pl.multiple_of(n * wide + lax.rem(r, 2) * short, short), short)]

    for c in range(nc):
        for side in range(2):
            base = side * 4
            for k in (1, 3, 2):
                two[c, side, k].wait_recv()
            v = s1[c, side, order_of(side)] + r2[c, base + 1] + r2[c, base + 2] + r2[c, base + 3]
            part = piece(c, block_of(side, 0), order_of(side))
            part[...] = v.astype(BF16)
            for k in (2, 1, 3):
                i = base + k
                three[c, side, k] = go(part, part, c_s.at[c, i], c_r.at[c, i], far(side, k))

    flush(6 * nc)

    def mirror(c, side, k):
        part = piece(c, block_of(side, 4 - k))
        i = side * 4 + k
        last[c].append(go(part, part, f_s.at[c, i], f_r.at[c, i], partner))

    for c in range(nc):
        for side in range(2):
            part = piece(c, block_of(side, 0))
            for k in (1, 3, 2):
                three[c, side, k].wait_recv()
            for k in (2, 1, 3):
                i = side * 4 + k
                four[c, side, k] = go(part, part, e_s.at[c, i], e_r.at[c, i], near(side, k))
            mirror(c, side, 0)
    flush(6 * nc)
    for c in range(nc):
        for k in (1, 3, 2):
            for side in range(2):
                four[c, side, k].wait_recv()
                mirror(c, side, k)
    flush(6 * nc)
    for c in range(nc):
        for cp in last[c]:
            cp.wait_recv()
    for cp in sends:
        cp.wait_send()


def solution(mesh):
    cache_spec = P('rep', 'seq', 'head', None)

    def local_step(tokens, w_query, w_key, w_value, w_out, k_cache, v_cache, positions):
        batch, shard, kv, dim = k_cache.shape
        model = tokens.shape[1]
        groups = w_query.shape[1] // w_key.shape[1]
        heads = kv * groups
        rows = shard * kv
        flat = (batch, rows, dim)
        hspec = pl.BlockSpec(memory_space=pltpu.HBM)
        anyspec = pl.BlockSpec(memory_space=pl.ANY)
        vspec = pl.BlockSpec(memory_space=pltpu.VMEM)
        dma = pltpu.SemaphoreType.DMA
        cache = jax.ShapeDtypeStruct(flat, BF16)
        blocks = groups + 2
        proj, kb, vb = pl.pallas_call(
            functools.partial(project, groups),
            out_shape=(jax.ShapeDtypeStruct((blocks, batch, kv * dim), BF16), cache, cache),
            in_specs=[hspec] * 6,
            out_specs=(vspec,) * 3,
            scratch_shapes=[pltpu.VMEM(tokens.shape, BF16), pltpu.VMEM((4, model // 4, kv * dim), BF16), dma,
                            dma((4,)), dma((8,)), dma((8,)), dma, dma],
            compiler_params=pltpu.CompilerParams(collective_id=1, has_side_effects=True, vmem_limit_bytes=16 << 20),
            cost_estimate=pl.CostEstimate(flops=10**10, bytes_accessed=30 * 10**6, transcendentals=0),
            name='project',
        )(*[pltpu.with_memory_space_constraint(a, pltpu.HBM) for a in (
            tokens, w_query, w_key, w_value, k_cache.reshape(flat), v_cache.reshape(flat))])
        k_new, v_new, _, _, acc, stat = pl.pallas_call(
            functools.partial(attend, groups),
            out_shape=(cache, cache, cache, cache, jax.ShapeDtypeStruct((heads, batch, dim), F32),
                       jax.ShapeDtypeStruct((PAD, dim), F32)),
            in_specs=[vspec, vspec, vspec, pl.BlockSpec(memory_space=pltpu.SMEM)],
            out_specs=(hspec, hspec, vspec, vspec, vspec, vspec),
            input_output_aliases={1: 2, 2: 3},
            scratch_shapes=[pltpu.VMEM((batch * PAD, dim), F32), pltpu.VMEM((2, batch, kv * dim), F32),
                            pltpu.VMEM((batch * PAD, dim), F32), pltpu.VMEM((2, rows, NB * PAD), F32),
                            dma((2, batch // NR))],
            compiler_params=pltpu.CompilerParams(vmem_limit_bytes=12 << 20),
            cost_estimate=pl.CostEstimate(flops=10**10, bytes_accessed=17 * 10**6, transcendentals=0),
            name='attend',
        )(proj, kb, vb, positions)

        wide = model // 8
        step = batch // 2 // NC
        ns = lax.axis_size('seq')
        y = pl.pallas_call(
            finish,
            out_shape=jax.ShapeDtypeStruct((8, 8, model), BF16),
            in_specs=[vspec, vspec, anyspec],
            out_specs=vspec,
            scratch_shapes=[
                pltpu.VMEM((2 * w_out.shape[0], model), BF16),
                pltpu.VMEM((ns // 2, NC, 2 * heads // ns, step, dim), F32),
                pltpu.VMEM((ns // 2, 8, dim), F32),
                pltpu.VMEM((8, dim), F32),
                pltpu.VMEM((NC, heads, step, dim), F32),
                pltpu.VMEM((NC, heads, step, dim), F32),
                pltpu.VMEM((dim, dim), F32),
                pltpu.VMEM((NC, step, 2 * w_out.shape[0]), BF16),
                pltpu.VMEM((NC, 8, step, wide), F32),
                pltpu.VMEM((NC, 8, step, wide), F32),
                pltpu.VMEM((NC, 2, 4, 8, wide // 2), F32),
                pltpu.VMEM((NC, 8, 8, wide // 2), F32),
                dma, dma, dma,
                dma((NC, 8)), dma((NC, 8)), dma((8,)), dma((8,)),
            ] + [dma((NC, 8))] * 10,
            compiler_params=pltpu.CompilerParams(collective_id=0, has_side_effects=True, vmem_limit_bytes=32 << 20),
            name='finish',
        )(acc, stat, w_out)
        return y.reshape(batch, model), k_new.reshape(k_cache.shape), v_new.reshape(v_cache.shape)

    return jax.shard_map(
        local_step,
        mesh=mesh,
        in_specs=(P('rep', None), P(), P(), P(), P(('head', 'seq'), None), cache_spec, cache_spec, P('rep')),
        out_specs=(P('rep', None), cache_spec, cache_spec),
        check_vma=False,
    )
```

```python
import functools

import jax
import jax.numpy as jnp
from jax import lax
from jax.experimental import pallas as pl
from jax.experimental.pallas import tpu as pltpu
from jax.sharding import PartitionSpec as P

MESH = pl.DeviceIdType.MESH
BF16 = jnp.bfloat16
F32 = jnp.float32
PAD = 16
NB = 16
NR = 8
NC = 2


def project(groups, tokens, wq, wk, wv, kc, vc, wo, pj, kb, vb, wob, tok, wbuf, tsem, wsem, ssem, rsem, ksem, vsem, osem):
    head = lax.axis_index('head')
    s = lax.axis_index('seq')
    ns = lax.axis_size('seq')
    parts, depth, width = wbuf.shape

    def load(i, src, block):
        rows = pl.ds(i * depth, depth)
        return pltpu.make_async_copy(src.at[rows, pl.ds(pl.multiple_of(block * width, width), width)], wbuf.at[i], wsem.at[i])

    first = pltpu.make_async_copy(tokens, tok, tsem)
    first.start()
    for i in range(parts):
        @pl.when(s < groups)
        def _():
            load(i, wq, head * groups + s).start()

        @pl.when(s == groups)
        def _():
            load(i, wk, head).start()

        @pl.when(s == groups + 1)
        def _():
            load(i, wv, head).start()

    wrows = wo.shape[0]
    mine = wob.at[pl.ds(pl.multiple_of(lax.rem(s, 2) * wrows, wrows), wrows), :]
    caches = [pltpu.make_async_copy(kc, kb, ksem), pltpu.make_async_copy(vc, vb, vsem),
              pltpu.make_async_copy(wo, mine, osem)]
    for cp in caches:
        cp.start()
    barrier = pltpu.get_barrier_semaphore()
    for k in range(1, ns):
        pl.semaphore_signal(barrier, inc=1, device_id={'head': head, 'seq': lax.rem(s + k, ns)}, device_id_type=MESH)
    first.wait()
    acc = jnp.zeros((tok.shape[0], width), F32)
    for i in range(parts):
        load(i, wq, 0).wait()
        acc = acc + jnp.dot(tok[:, i * depth:(i + 1) * depth], wbuf[i], preferred_element_type=F32)
    pj[s] = acc.astype(BF16)
    pl.semaphore_wait(barrier, ns - 1)
    sends = []
    for k in (4, 5, 3, 2, 6, 7, 1):
        cp = pltpu.make_async_remote_copy(src_ref=pj.at[s], dst_ref=pj.at[s], send_sem=ssem.at[k], recv_sem=rsem.at[k],
                                          device_id={'head': head, 'seq': lax.rem(s + k, ns)}, device_id_type=MESH)
        cp.start()
        sends.append(cp)
    cp = pltpu.make_async_remote_copy(src_ref=wo, dst_ref=mine, send_sem=ssem.at[0], recv_sem=rsem.at[0],
                                      device_id={'head': head, 'seq': s + 1 - 2 * lax.rem(s, 2)}, device_id_type=MESH)
    cp.start()
    sends.append(cp)
    for cp in sends:
        cp.wait_recv()
    for cp in sends:
        cp.wait_send()
    for cp in caches:
        cp.wait()


def attend(groups, pj, kin, vin, pos, ko, vo, kb, vb, acch, stat, q2, nkv, accs, sb, osem):
    seq = lax.axis_index('seq')
    batch, rows, dim = kb.shape
    shard = rows // 2
    heads = 2 * groups
    steps = batch // NB
    nkv[0] = pj[groups].astype(F32)
    nkv[1] = pj[groups + 1].astype(F32)

    row16 = lax.broadcasted_iota(jnp.int32, (16, dim), 0)
    even = (row16 & 1) == 0
    lanes = NB * PAD
    lane = lax.broadcasted_iota(jnp.int32, (8, lanes), 1)
    sub = lax.broadcasted_iota(jnp.int32, (8, lanes), 0)
    hl = lane & (PAD - 1)
    match = jnp.where(hl < groups, 0, jnp.where(hl < heads, 1, 2)) == (sub & 1)
    tile = lax.broadcasted_iota(jnp.int32, (rows // 8, 8, lanes), 0) * 4

    def out(j, c):
        span = pl.ds(pl.multiple_of(c * NR, NR), NR)
        src, dst = ((kb, ko), (vb, vo))[j]
        return pltpu.make_async_copy(src.at[span], dst.at[span], osem.at[j, c])

    def refresh(c, carry):
        fresh = []
        for i in range(NR):
            b = c * NR + i
            t = pos[b] - seq * shard
            inside = (t >= 0) & (t < shard)
            tc = jnp.clip(t, 0, shard - 1)
            start = pl.multiple_of((tc >> 3) * 16, 16)
            hit = ((row16 >> 1) == (tc & 7)) & inside
            for j, buf in enumerate((kb, vb)):
                new = nkv[j, pl.ds(b, 1), :]
                new = jnp.where(even, new[:, :dim], new[:, dim:])
                old = buf[b, pl.ds(start, 16), :].astype(F32)
                fresh.append((buf, b, start, jnp.where(hit, new, old).astype(BF16)))
        for buf, b, start, value in fresh:
            buf[b, pl.ds(start, 16), :] = value
        out(0, c).start()
        out(1, c).start()
        return carry

    lax.fori_loop(0, batch // NR, refresh, 0)
    q2[...] = jnp.zeros_like(q2)
    for h in range(heads):
        q2[pl.ds(h, batch, stride=PAD), :] = pj[h // 2][:, (h % 2) * dim:(h % 2 + 1) * dim].astype(F32)
    ql = lax.broadcasted_iota(jnp.int32, (dim, lanes), 1) // PAD

    def scores(c):
        qt = jnp.transpose(q2[c * lanes:(c + 1) * lanes, :]).astype(BF16)
        zero = jnp.zeros_like(qt)
        s = jnp.zeros((rows, lanes), F32)
        for j in range(NB // 2):
            b = c * NB + 2 * j
            lhs = jnp.concatenate([kb[b], kb[b + 1]], axis=1)
            rhs = jnp.concatenate([jnp.where(ql == 2 * j, qt, zero), jnp.where(ql == 2 * j + 1, qt, zero)], axis=0)
            s = s + jnp.dot(lhs, rhs, preferred_element_type=F32)
        sb[c % 2] = s

    def mix(c):
        limit = jnp.zeros((8, lanes), jnp.int32)
        for i in range(NB):
            limit = jnp.where(lane // PAD == i, pos[c * NB + i] - seq * shard, limit)
        edge = jnp.where(match, limit, -1) - (sub >> 1)
        s = sb[c % 2].reshape(rows // 8, 8, lanes) * dim ** -0.5
        s = jnp.where(tile <= edge[None], s, -jnp.inf)
        m = jnp.max(jnp.max(s, axis=0), axis=0, keepdims=True)
        w = jnp.exp(s - jnp.where(m == -jnp.inf, 0.0, m)[None])
        l = jnp.sum(jnp.sum(w, axis=0), axis=0, keepdims=True)
        for r in range(lanes // dim):
            g = c * (lanes // dim) + r
            g = g // 4 * 8 + g % 4
            stat[g:g + 1, :] = m[:, r * dim:(r + 1) * dim]
            stat[g + 4:g + 5, :] = l[:, r * dim:(r + 1) * dim]
        wt = jnp.transpose(w.reshape(rows, lanes).astype(BF16))
        for j in range(NB // 2):
            b = c * NB + 2 * j
            rhs = jnp.concatenate([vb[b], vb[b + 1]], axis=1)
            a = jnp.dot(wt[2 * PAD * j:2 * PAD * (j + 1)], rhs, preferred_element_type=F32)
            accs[b * PAD:(b + 1) * PAD, :] = a[:PAD, :dim]
            accs[(b + 1) * PAD:(b + 2) * PAD, :] = a[PAD:, dim:]

    scores(0)
    for c in range(steps):
        if c + 1 < steps:
            scores(c + 1)
        mix(c)
    for h in range(heads):
        acch[h] = accs[pl.ds(h, batch, stride=PAD), :]
    for c in range(batch // NR):
        out(0, c).wait()
        out(1, c).wait()


def finish(acch, stat, wob, out, rx, srx, sx, dx, pr, fs, lhs, z, r1, s1, r2,
           d_s, d_r, t_s, t_r, a_s, a_r, b_s, b_r, c_s, c_r, e_s, e_r, f_s, f_r):
    y = lax.axis_index('head')
    s = lax.axis_index('seq')
    ny = lax.axis_size('head')
    ns = lax.axis_size('seq')
    nx = ns // 2
    x = s // 2
    p = lax.rem(s, 2)
    heads, batch, dim = acch.shape
    nc, per, step = rx.shape[1:4]
    half = nc * step
    wide = z.shape[-1]
    short = wide // 2

    def on_x(k):
        return {'head': y, 'seq': lax.rem(x + k, nx) * 2 + p}

    def on_y(k):
        return {'head': lax.rem(y + k, ny), 'seq': s}

    def copy(src, dst, send, recv, dev):
        return pltpu.make_async_remote_copy(src_ref=src, dst_ref=dst, send_sem=send, recv_sem=recv,
                                            device_id=dev, device_id_type=MESH)

    partner = {'head': y, 'seq': x * 2 + 1 - p}
    barrier = pltpu.get_barrier_semaphore()
    for k in (2, 1, 3):
        pl.semaphore_signal(barrier, inc=1, device_id=on_x(k), device_id_type=MESH)
        pl.semaphore_signal(barrier, inc=1, device_id=on_y(k), device_id_type=MESH)
    pl.semaphore_signal(barrier, inc=1, device_id=partner, device_id_type=MESH)
    pl.semaphore_wait(barrier, 7)

    sends = []

    def go(*a):
        cp = copy(*a)
        cp.start()
        sends.append(cp)
        return cp

    def flush(n):
        for cp in sends[:n]:
            cp.wait_send()
        del sends[:n]

    there, here = 1 - p, p
    scopy = go(stat.at[pl.ds(pl.multiple_of(there * 8, 8), 8)], sx, t_s.at[0], t_r.at[0], partner)
    pairs = []
    for c in range(nc):
        rows = pl.ds(pl.multiple_of(there * half + c * step, step), step)
        pairs.append(go(acch.at[:, rows], dx.at[c], d_s.at[c, 0], d_r.at[c, 0], partner))
    n8 = half // 8
    fs[...] = jnp.zeros_like(fs)
    ours = stat[pl.ds(pl.multiple_of(here * 8, 8), 8)]
    scopy.wait_recv()
    theirs = sx[...]
    peak = jnp.maximum(ours[:n8], theirs[:n8])
    base = jnp.where(peak == -jnp.inf, 0.0, peak)
    scale = [jnp.exp(t[:n8] - base) for t in (ours, theirs)]
    srx[0, :n8] = peak
    srx[0, n8:] = scale[0] * ours[n8:] + scale[1] * theirs[n8:]
    stats = [go(srx.at[0], srx.at[k], t_s.at[k], t_r.at[k], on_x(k)) for k in (2, 1, 3)]
    fs[:n8] = scale[0]
    fs[n8:2 * n8] = scale[1]
    fs[...] = jnp.transpose(fs[...])
    parts = {}
    for c in range(nc):
        pairs[c].wait_recv()
        for h in range(heads):
            col = fs[pl.ds(h, 8, stride=PAD), :]
            for g in range(step // 8):
                lead = c * (step // 8) + g
                pr[c, h, 8 * g:8 * g + 8] = (col[:, lead:lead + 1] * acch[h, pl.ds(half * here + 8 * lead, 8)]
                                             + col[:, n8 + lead:n8 + lead + 1] * dx[c, h, 8 * g:8 * g + 8])
        parts[c] = [go(pr.at[c, pl.ds(lax.rem(x + k, nx) * per, per)], rx.at[k, c], d_s.at[c, k], d_r.at[c, k], on_x(k))
                    for k in (2, 1, 3)]

    fs[...] = jnp.zeros_like(fs)
    for cp in stats:
        cp.wait_recv()
    top = functools.reduce(jnp.maximum, [srx[i, :n8] for i in range(nx)])
    scale = [jnp.exp(srx[i, :n8] - top) for i in range(nx)]
    total = functools.reduce(lambda a, b: a + b, [e * srx[i, n8:] for i, e in enumerate(scale)])
    for i in range(nx):
        fs[i * n8:(i + 1) * n8, :] = scale[i] / total
    fs[...] = jnp.transpose(fs[...])

    def block_of(side, k):
        return lax.rem(x + k, nx) if side == 0 else nx + lax.rem(y + k, ny)

    def near(side, k):
        return on_x(k) if side == 0 else on_y(k)

    def far(side, k):
        return on_y(k) if side == 0 else on_x(k)

    def order_of(side):
        return y if side == 0 else x

    early = len(sends)
    cols = [fs[pl.ds(x * per + j, 8, stride=PAD), :] for j in range(per)]
    one, two, three, four, last = {}, {}, {}, {}, {c: [] for c in range(nc)}
    for c in range(nc):
        for cp in parts[c]:
            cp.wait_recv()
        for j in range(per):
            rows = []
            for g in range(step // 8):
                lead = c * (step // 8) + g
                acc = cols[j][:, lead:lead + 1] * pr[c, x * per + j, 8 * g:8 * g + 8]
                for i in range(1, nx):
                    acc = acc + cols[j][:, i * n8 + lead:i * n8 + lead + 1] * rx[i, c, j, 8 * g:8 * g + 8]
                rows.append(acc)
            lhs[c, :, j * dim:(j + 1) * dim] = jnp.concatenate(rows, axis=0).astype(BF16)
        for k in (2, 1, 3, 0):
            for side in range(2):
                n = block_of(side, k)
                z[c, side * 4 + k] = jnp.dot(lhs[c], wob[:, pl.ds(pl.multiple_of(n * wide, wide), wide)],
                                             preferred_element_type=F32)
            for side in range(2 if k else 0):
                i = side * 4 + k
                one[c, side, k] = go(z.at[c, i], r1.at[c, i], a_s.at[c, i], a_r.at[c, i], near(side, k))

    for c in range(nc):
        for side in range(2):
            base = side * 4
            for k in (1, 3, 2):
                one[c, side, k].wait_recv()
            v = z[c, base] + r1[c, base + 1] + r1[c, base + 2] + r1[c, base + 3]
            for r in range(4):
                s1[c, side, r] = v[8 * (r // 2):8 * (r // 2) + 8, short * (r % 2):short * (r % 2 + 1)]
            for k in (2, 1, 3):
                dest = lax.rem(order_of(side) + k, 4)
                i = base + k
                two[c, side, k] = go(s1.at[c, side, dest], r2.at[c, i], b_s.at[c, i], b_r.at[c, i], far(side, k))

    flush(early)

    def piece(c, n, r=None):
        row = 4 * p + 2 * c
        if r is None:
            return out.at[pl.ds(row, 2), :, pl.ds(pl.multiple_of(n * wide, wide), wide)]
        return out.at[row + r // 2, :, pl.ds(pl.multiple_of(n * wide + lax.rem(r, 2) * short, short), short)]

    for c in range(nc):
        for side in range(2):
            base = side * 4
            for k in (1, 3, 2):
                two[c, side, k].wait_recv()
            v = s1[c, side, order_of(side)] + r2[c, base + 1] + r2[c, base + 2] + r2[c, base + 3]
            part = piece(c, block_of(side, 0), order_of(side))
            part[...] = v.astype(BF16)
            for k in (2, 1, 3):
                i = base + k
                three[c, side, k] = go(part, part, c_s.at[c, i], c_r.at[c, i], far(side, k))

    flush(6 * nc)

    def mirror(c, side, k):
        part = piece(c, block_of(side, 4 - k))
        i = side * 4 + k
        last[c].append(go(part, part, f_s.at[c, i], f_r.at[c, i], partner))

    for c in range(nc):
        for side in range(2):
            part = piece(c, block_of(side, 0))
            for k in (1, 3, 2):
                three[c, side, k].wait_recv()
            for k in (2, 1, 3):
                i = side * 4 + k
                four[c, side, k] = go(part, part, e_s.at[c, i], e_r.at[c, i], near(side, k))
            mirror(c, side, 0)
    flush(6 * nc)
    for c in range(nc):
        for k in (1, 3, 2):
            for side in range(2):
                four[c, side, k].wait_recv()
                mirror(c, side, k)
    flush(6 * nc)
    for c in range(nc):
        for cp in last[c]:
            cp.wait_recv()
    for cp in sends:
        cp.wait_send()


def solution(mesh):
    cache_spec = P('rep', 'seq', 'head', None)

    def local_step(tokens, w_query, w_key, w_value, w_out, k_cache, v_cache, positions):
        batch, shard, kv, dim = k_cache.shape
        model = tokens.shape[1]
        groups = w_query.shape[1] // w_key.shape[1]
        heads = kv * groups
        rows = shard * kv
        flat = (batch, rows, dim)
        hspec = pl.BlockSpec(memory_space=pltpu.HBM)
        anyspec = pl.BlockSpec(memory_space=pl.ANY)
        vspec = pl.BlockSpec(memory_space=pltpu.VMEM)
        dma = pltpu.SemaphoreType.DMA
        cache = jax.ShapeDtypeStruct(flat, BF16)
        blocks = groups + 2
        proj, kb, vb, wob = pl.pallas_call(
            functools.partial(project, groups),
            out_shape=(jax.ShapeDtypeStruct((blocks, batch, kv * dim), BF16), cache, cache,
                       jax.ShapeDtypeStruct((2 * w_out.shape[0], model), BF16)),
            in_specs=[hspec] * 7,
            out_specs=(vspec,) * 4,
            scratch_shapes=[pltpu.VMEM(tokens.shape, BF16), pltpu.VMEM((4, model // 4, kv * dim), BF16), dma,
                            dma((4,)), dma((8,)), dma((8,)), dma, dma, dma],
            compiler_params=pltpu.CompilerParams(collective_id=1, has_side_effects=True, vmem_limit_bytes=16 << 20),
            cost_estimate=pl.CostEstimate(flops=10**10, bytes_accessed=30 * 10**6, transcendentals=0),
            name='project',
        )(*[pltpu.with_memory_space_constraint(a, pltpu.HBM) for a in (
            tokens, w_query, w_key, w_value, k_cache.reshape(flat), v_cache.reshape(flat), w_out)])
        k_new, v_new, _, _, acc, stat = pl.pallas_call(
            functools.partial(attend, groups),
            out_shape=(cache, cache, cache, cache, jax.ShapeDtypeStruct((heads, batch, dim), F32),
                       jax.ShapeDtypeStruct((PAD, dim), F32)),
            in_specs=[vspec, vspec, vspec, pl.BlockSpec(memory_space=pltpu.SMEM)],
            out_specs=(hspec, hspec, vspec, vspec, vspec, vspec),
            input_output_aliases={1: 2, 2: 3},
            scratch_shapes=[pltpu.VMEM((batch * PAD, dim), F32), pltpu.VMEM((2, batch, kv * dim), F32),
                            pltpu.VMEM((batch * PAD, dim), F32), pltpu.VMEM((2, rows, NB * PAD), F32),
                            dma((2, batch // NR))],
            compiler_params=pltpu.CompilerParams(vmem_limit_bytes=12 << 20),
            cost_estimate=pl.CostEstimate(flops=10**10, bytes_accessed=17 * 10**6, transcendentals=0),
            name='attend',
        )(proj, kb, vb, positions)

        wide = model // 8
        step = batch // 2 // NC
        ns = lax.axis_size('seq')
        y = pl.pallas_call(
            finish,
            out_shape=jax.ShapeDtypeStruct((8, 8, model), BF16),
            in_specs=[vspec, vspec, vspec],
            out_specs=vspec,
            scratch_shapes=[
                pltpu.VMEM((ns // 2, NC, 2 * heads // ns, step, dim), F32),
                pltpu.VMEM((ns // 2, 8, dim), F32),
                pltpu.VMEM((8, dim), F32),
                pltpu.VMEM((NC, heads, step, dim), F32),
                pltpu.VMEM((NC, heads, step, dim), F32),
                pltpu.VMEM((dim, dim), F32),
                pltpu.VMEM((NC, step, 2 * w_out.shape[0]), BF16),
                pltpu.VMEM((NC, 8, step, wide), F32),
                pltpu.VMEM((NC, 8, step, wide), F32),
                pltpu.VMEM((NC, 2, 4, 8, wide // 2), F32),
                pltpu.VMEM((NC, 8, 8, wide // 2), F32),
                dma((NC, 8)), dma((NC, 8)), dma((8,)), dma((8,)),
            ] + [dma((NC, 8))] * 10,
            compiler_params=pltpu.CompilerParams(collective_id=0, has_side_effects=True, vmem_limit_bytes=32 << 20),
            name='finish',
        )(acc, stat, wob)
        return y.reshape(batch, model), k_new.reshape(k_cache.shape), v_new.reshape(v_cache.shape)

    return jax.shard_map(
        local_step,
        mesh=mesh,
        in_specs=(P('rep', None), P(), P(), P(), P(('head', 'seq'), None), cache_spec, cache_spec, P('rep')),
        out_specs=(P('rep', None), cache_spec, cache_spec),
        check_vma=False,
    )
```
